32 devices in a mesh: dp: 1 (over z), etp: 4 (over y), ep: 8 (over x, core).
Axes of the slice: x: 4, y: 4, z: 1, core: 2. Of those that a mesh axis runs over, the one named last changes fastest.
The devices are a block of a 4x4x8 slice.
Arguments:
- hidden: bfloat16 [16384, 1024], P(('dp', 'ep'))
- expert_ids: int32 [16384, 8], P(('dp', 'ep'))
- gate_wts: float32 [16384, 8], P(('dp', 'ep'))
- slot_pos: int32 [16384, 8], P(('dp', 'ep'))
- w_gate: bfloat16 [32, 1024, 512], P('ep', None, 'etp')
- w_up: bfloat16 [32, 1024, 512], P('ep', None, 'etp')
- w_down: bfloat16 [32, 512, 1024], P('ep', 'etp')
Outputs:
- output: bfloat16 [16384, 1024], P(('dp', 'ep'))
All inputs are finite; a program needn't handle non-finite values.
Results may differ from the reference program's by a relative error of at most 0.001.
Values are sent between devices in bfloat16 or wider.
A program may use at most 768 MiB of HBM per device.

```python
import jax
import jax.numpy as jnp
from jax import lax

D_MODEL = 1024
D_FF = 512
EXPERTS = 32
TOP_K = 8
TOK_DEV = 2048
GROUP = 8
LOCAL_CAP = 640

TOKENS = TOK_DEV * GROUP
CAPACITY = LOCAL_CAP * GROUP


def rank_in_expert(flat_ids, priority):
    n_choices = flat_ids.shape[0]
    sort_order = jnp.argsort(flat_ids * n_choices + priority)
    sorted_ids = flat_ids[sort_order]
    counts = jnp.bincount(flat_ids, length=EXPERTS)
    starts = jnp.cumsum(counts) - counts
    sorted_rank = jnp.arange(n_choices) - starts[sorted_ids]
    return jnp.zeros((n_choices,), jnp.int32).at[sort_order].set(sorted_rank.astype(jnp.int32))


def draw_routing(route_key):
    key_hot, key_rows, key_bias, key_score, key_prio = jax.random.split(route_key, 5)
    hot_expert = jax.random.randint(key_hot, (GROUP,), 0, EXPERTS)
    row_perm = jax.vmap(lambda sub_key: jax.random.permutation(sub_key, TOK_DEV))(jax.random.split(key_rows, GROUP))
    forced = row_perm < LOCAL_CAP
    expert_bias = jax.random.randint(key_bias, (EXPERTS,), 0, 2 ** 19)
    scores = jax.random.randint(key_score, (GROUP, TOK_DEV, EXPERTS), 0, 2 ** 20) + expert_bias
    expert_range = jnp.arange(EXPERTS)
    is_hot = forced[:, :, None] & (expert_range[None, None, :] == hot_expert[:, None, None])
    scores = jnp.where(is_hot, 2 ** 21, scores)
    top_scores, expert_ids = lax.top_k(scores * EXPERTS + expert_range, TOP_K)
    priority = jax.vmap(lambda sub_key: jax.random.permutation(sub_key, TOK_DEV * TOP_K))(jax.random.split(key_prio, GROUP))
    local_rank = jax.vmap(rank_in_expert)(expert_ids.reshape(GROUP, TOK_DEV * TOP_K), priority)
    block_base = (jnp.arange(GROUP) * LOCAL_CAP)[:, None]
    slot_pos = jnp.where(local_rank < LOCAL_CAP, block_base + local_rank, -1)
    return expert_ids.reshape(TOKENS, TOP_K).astype(jnp.int32), slot_pos.reshape(TOKENS, TOP_K).astype(jnp.int32)


def setup_inputs(seed: int = 0, part: int = 0) -> dict:
    base_key = jax.random.key(seed)
    part_key = jax.random.fold_in(base_key, part)
    key_hidden, key_route, key_gate = jax.random.split(part_key, 3)
    key_w_gate, key_w_up, key_w_down = jax.random.split(jax.random.key(seed + 1), 3)
    hidden = jax.random.normal(key_hidden, (TOKENS, D_MODEL), jnp.float32).astype(jnp.bfloat16)
    expert_ids, slot_pos = draw_routing(key_route)
    logits = jax.random.normal(key_gate, (TOKENS, TOP_K), jnp.float32)
    gate_wts = jax.nn.softmax(logits, axis=-1)
    w_gate = (jax.random.normal(key_w_gate, (EXPERTS, D_MODEL, D_FF), jnp.float32) * D_MODEL ** -0.5).astype(jnp.bfloat16)
    w_up = (jax.random.normal(key_w_up, (EXPERTS, D_MODEL, D_FF), jnp.float32) * D_MODEL ** -0.5).astype(jnp.bfloat16)
    w_down = (jax.random.normal(key_w_down, (EXPERTS, D_FF, D_MODEL), jnp.float32) * D_FF ** -0.5).astype(jnp.bfloat16)
    return dict(hidden=hidden, expert_ids=expert_ids, gate_wts=gate_wts, slot_pos=slot_pos, w_gate=w_gate, w_up=w_up, w_down=w_down)


def reference(hidden, expert_ids, gate_wts, slot_pos, w_gate, w_up, w_down):
    flat_pos = slot_pos.reshape(-1)
    slot_index = jnp.where(flat_pos >= 0, expert_ids.reshape(-1) * CAPACITY + flat_pos, EXPERTS * CAPACITY)
    token_index = jnp.broadcast_to(jnp.arange(TOKENS, dtype=jnp.int32)[:, None], (TOKENS, TOP_K)).reshape(-1)
    slot_token = jnp.full((EXPERTS * CAPACITY,), TOKENS, jnp.int32).at[slot_index].set(token_index, mode='drop')
    slot_gate = jnp.zeros((EXPERTS * CAPACITY,), jnp.float32).at[slot_index].set(gate_wts.reshape(-1), mode='drop')

    def expert_step(running, operands):
        tok_ids, gate_col, gate_mat, up_mat, down_mat = operands
        buffer = jnp.take(hidden, tok_ids, axis=0, mode='fill', fill_value=0)
        h_gate = jnp.dot(buffer, gate_mat, preferred_element_type=jnp.float32)
        h_up = jnp.dot(buffer, up_mat, preferred_element_type=jnp.float32)
        hidden_act = (jax.nn.silu(h_gate) * h_up).astype(jnp.bfloat16)
        expert_out = jnp.dot(hidden_act, down_mat, preferred_element_type=jnp.float32)
        running = running + jax.ops.segment_sum(expert_out * gate_col[:, None], tok_ids, num_segments=TOKENS)
        return running, None

    start_sum = jnp.zeros((TOKENS, D_MODEL), jnp.float32)
    total_out, unused = lax.scan(expert_step, start_sum, (slot_token.reshape(EXPERTS, CAPACITY), slot_gate.reshape(EXPERTS, CAPACITY), w_gate, w_up, w_down))
    return total_out.astype(jnp.bfloat16)
```

```python
import functools

import jax
import jax.numpy as jnp
from jax import lax
from jax.experimental import pallas as pl
from jax.experimental.pallas import tpu as pltpu
from jax.sharding import PartitionSpec as P


def experts_kernel(tok_ref, gate_ref, wgu_ref, wdn_ref, out_ref, act_ref):
    n_q, n_e, d_model, two_f = wgu_ref.shape
    half = two_f // 2
    for e in range(n_e):
        gate = gate_ref[:, e:e + 1]
        for q in range(n_q):
            gu = jnp.dot(tok_ref[...], wgu_ref[q, e], preferred_element_type=jnp.float32)
            h_gate = gu[:, :half]
            act = jnp.where(gate > 0, jax.nn.silu(h_gate) * gu[:, half:], 0.0)
            act_ref[:, q * half:(q + 1) * half] = act.astype(jnp.bfloat16)
        down = wdn_ref[:, e].reshape(n_q * half, d_model)
        term = gate * jnp.dot(act_ref[...], down, preferred_element_type=jnp.float32)
        if e == 0:
            out_ref[...] = term
        else:
            out_ref[...] += term


def solution(mesh):
    row_spec = P(('dp', 'ep'), None)
    col_spec = P('ep', None, 'etp')
    in_specs = (row_spec, row_spec, row_spec, row_spec, col_spec, col_spec, P('ep', 'etp', None))
    n_q = mesh.shape['etp']
    group = mesh.shape['ep']

    def device_step(hidden, expert_ids, gate_wts, slot_pos, w_gate, w_up, w_down):
        rows_dev, d_model = hidden.shape
        n_e = w_gate.shape[0]
        width = w_gate.shape[2]
        rows = rows_dev // n_q
        start = lax.axis_index('etp') * rows
        cut = lambda a: lax.dynamic_slice_in_dim(a, start, rows, axis=0)
        ids, gts, pos = cut(expert_ids), cut(gate_wts), cut(slot_pos)
        hit = (ids[:, :, None] == jnp.arange(n_e * group, dtype=jnp.int32)[None, None, :]) & (pos >= 0)[:, :, None]
        dense = jnp.sum(jnp.where(hit, gts[:, :, None], 0.0), axis=1)
        all_gates = lax.all_gather(dense, 'ep', axis=0, tiled=True)
        gates = lax.dynamic_slice_in_dim(all_gates, lax.axis_index('ep') * n_e, n_e, axis=1)
        tok = lax.all_gather(cut(hidden), 'ep', axis=0, tiled=True)
        wgu = lax.all_gather(jnp.concatenate([w_gate, w_up], axis=-1), 'etp')
        wdn = lax.all_gather(w_down, 'etp')
        n_tok = rows * group
        part = pl.pallas_call(
            experts_kernel,
            out_shape=jax.ShapeDtypeStruct((n_tok, d_model), jnp.float32),
            grid=(group,),
            in_specs=[
                pl.BlockSpec((rows, d_model), lambda i: (i, 0)),
                pl.BlockSpec((rows, n_e), lambda i: (i, 0)),
                pl.BlockSpec((n_q, n_e, d_model, 2 * width), lambda i: (0, 0, 0, 0)),
                pl.BlockSpec((n_q, n_e, width, d_model), lambda i: (0, 0, 0, 0)),
            ],
            out_specs=pl.BlockSpec((rows, d_model), lambda i: (i, 0)),
            scratch_shapes=[pltpu.VMEM((rows, n_q * width), jnp.bfloat16)],
            compiler_params=pltpu.CompilerParams(vmem_limit_bytes=60 * 1024 * 1024),
            cost_estimate=pl.CostEstimate(flops=6 * n_tok * n_e * d_model * n_q * width, bytes_accessed=8 * n_tok * d_model, transcendentals=0),
        )(tok, gates, wgu, wdn)
        own = lax.psum_scatter(part, 'ep', scatter_dimension=0, tiled=True)
        return lax.all_gather(own.astype(jnp.bfloat16), 'etp', axis=0, tiled=True)

    return jax.shard_map(device_step, mesh=mesh, in_specs=in_specs, out_specs=row_spec, check_vma=False)
```

```python
import functools

import jax
import jax.numpy as jnp
from jax import lax
from jax.experimental import pallas as pl
from jax.experimental.pallas import tpu as pltpu
from jax.sharding import PartitionSpec as P

MESH = pl.DeviceIdType.MESH
CHUNKS = 4


def moe_kernel(n_q, group, hid, gat, wg, wu, wd, out, tok, gts, wgu, wdn, act, spart, pr, acc, r1, r2, fin, ssem, rsem, lsem, credit):
    rows, d_model = tok.shape[1:]
    n_e, width = wg.shape[0], wg.shape[2]
    cw = d_model // CHUNKS
    nx = group // 2
    hr, hk, he = rows // 2, d_model // 2, n_e // 2
    q, ep = lax.axis_index('etp'), lax.axis_index('ep')
    x, c = lax.div(ep, 2), lax.rem(ep, 2)
    yl, yr = lax.rem(q + n_q - 1, n_q), lax.rem(q + 1, n_q)
    xl, xr, xf = lax.rem(x + nx - 1, nx), lax.rem(x + 1, nx), lax.rem(x + 2, nx)
    bl, br, bf = xl * 2 + c, xr * 2 + c, xf * 2 + c
    to_l, to_r, to_p = {'ep': bl}, {'ep': br}, {'ep': x * 2 + 1 - c}
    up_l, up_r = {'etp': yl}, {'etp': yr}
    used = [0, 0]
    sends, locals_ = [], []

    def remote(src, dst, dev):
        k = used[0]
        used[0] += 1
        cp = pltpu.make_async_remote_copy(src_ref=src, dst_ref=dst, send_sem=ssem.at[k], recv_sem=rsem.at[k], device_id=dev, device_id_type=MESH)
        cp.start()
        sends.append(cp)
        return cp

    def local(src, dst):
        k = used[1]
        used[1] += 1
        cp = pltpu.make_async_copy(src, dst, lsem.at[k])
        cp.start()
        return cp

    barrier = pltpu.get_barrier_semaphore()
    for dev in (to_l, to_r, to_p, up_l, up_r):
        pl.semaphore_signal(barrier, inc=1, device_id=dev, device_id_type=MESH)
    pl.semaphore_wait(barrier, 5)

    def send_gu(e):
        cps = []
        for dev in (up_r, up_l):
            cps.append(remote(wg.at[e], wgu.at[e, q, :, 0:width], dev))
            cps.append(remote(wu.at[e], wgu.at[e, q, :, width:2 * width], dev))
        return cps

    def pass_gu(e, cps):
        for cp in cps:
            cp.wait_recv()
        return [
            remote(wgu.at[e, yl, 0:hk], wgu.at[e, yl, 0:hk], up_r),
            remote(wgu.at[e, yr, hk:d_model], wgu.at[e, yr, hk:d_model], up_l),
        ]

    def send_dn(n):
        return [remote(wd.at[:, :, n * cw:(n + 1) * cw], wdn.at[n, :, q], dev) for dev in (up_r, up_l)]

    def pass_dn(n, cps):
        for cp in cps:
            cp.wait_recv()
        return [
            remote(wdn.at[n, 0:he, yl], wdn.at[n, 0:he, yl], up_r),
            remote(wdn.at[n, he:n_e, yr], wdn.at[n, he:n_e, yr], up_l),
        ]

    def arrive(cps):
        for cp in cps:
            cp.wait_recv()

    own_rows = hid.at[pl.ds(pl.multiple_of(q * rows, rows), rows)]
    gu = {0: send_gu(0)}
    tok_p = [remote(own_rows, tok.at[ep], to_p), remote(gat, gts.at[ep], to_p)]
    tok_r = [remote(own_rows, tok.at[ep], to_r), remote(gat, gts.at[ep], to_r)]
    tok_l = [remote(own_rows, tok.at[ep], to_l), remote(gat, gts.at[ep], to_l)]
    gu[1] = send_gu(1)
    mine = [local(own_rows, tok.at[ep]), local(gat, gts.at[ep])]
    for e in range(n_e):
        mine.append(local(wg.at[e], wgu.at[e, q, :, 0:width]))
        mine.append(local(wu.at[e], wgu.at[e, q, :, width:2 * width]))
    for n in range(CHUNKS):
        mine.append(local(wd.at[:, :, n * cw:(n + 1) * cw], wdn.at[n, :, q]))

    fwd, dn, fdn = {}, {}, {}
    fwd[0] = pass_gu(0, gu[0])
    gu[2] = send_gu(2)
    arrive(tok_r)
    arrive(tok_l)
    far = [
        remote(tok.at[bl, 0:hr], tok.at[bl, 0:hr], to_r),
        remote(gts.at[bl], gts.at[bl], to_r),
        remote(tok.at[br, hr:rows], tok.at[br, hr:rows], to_l),
    ]
    relay = [remote(tok.at[b], tok.at[b], to_p) for b in (bl, br)]
    relay += [remote(gts.at[b], gts.at[b], to_p) for b in (bl, br)]
    fwd[1] = pass_gu(1, gu[1])
    gu[3] = send_gu(3)
    arrive(far)
    relay += [remote(tok.at[bf], tok.at[bf], to_p), remote(gts.at[bf], gts.at[bf], to_p)]
    fwd[2] = pass_gu(2, gu[2])
    dn[0] = send_dn(0)
    for cp in mine:
        cp.wait()
    arrive(tok_p)
    arrive(relay)

    def gates_of(b):
        return gts[b, ep].T

    def up_phase(e):
        arrive(fwd[e])

        def body(b, carry):
            gate = gates_of(b)[:, e:e + 1]
            for j in range(n_q):
                prod = jnp.dot(tok[b], wgu[e, j], preferred_element_type=jnp.float32)
                h = jnp.where(gate > 0, jax.nn.silu(prod[:, :width]) * prod[:, width:], 0.0)
                act[b * n_e + e, :, j * width:(j + 1) * width] = h.astype(jnp.bfloat16)
            return carry

        lax.fori_loop(0, group, body, 0)

    up_phase(0)
    up_phase(1)
    fwd[3] = pass_gu(3, gu[3])
    dn[1] = send_dn(1)
    up_phase(2)
    fdn[0] = pass_dn(0, dn[0])
    dn[2] = send_dn(2)
    up_phase(3)
    fdn[1] = pass_dn(1, dn[1])
    dn[3] = send_dn(3)

    def down(n, b, dst):
        gate = gates_of(b)
        for e in range(n_e):
            mat = wdn[n, e].reshape(n_q * width, cw)
            term = gate[:, e:e + 1] * jnp.dot(act[b * n_e + e], mat, preferred_element_type=jnp.float32)
            if e == 0:
                dst[...] = term
            else:
                dst[...] += term

    d2d, first, second, outs, fouts = {}, {}, {}, {}, {}

    def phase_a(n):
        arrive(fdn[n])
        if n >= 1:
            d2d[n - 1].wait_send()
            sends[:] = [cp for cp in sends if cp is not d2d[n - 1]]

        def other(i, carry):
            xi = lax.rem(xf + i, nx)
            down(n, xi * 2 + 1 - c, spart.at[xi])
            return carry

        lax.fori_loop(0, nx, other, 0)
        if n >= 2:
            pl.semaphore_wait(credit.at[n % 2], 1)
        d2d[n] = remote(spart, pr.at[n % 2], to_p)

        def own(i, carry):
            xi = lax.rem(xf + i, nx)
            down(n, xi * 2 + c, acc.at[n, xi])
            return carry

        lax.fori_loop(0, nx, own, 0)

    def phase_b(n):
        d2d[n].wait_recv()
        acc[n, xf] += pr[n % 2, xf]
        first[n] = [
            remote(acc.at[n, xf, 0:hr], r1.at[n, 0], to_r),
            remote(acc.at[n, xf, hr:rows], r1.at[n, 1], to_l),
        ]
        acc[n, xr] += pr[n % 2, xr]
        acc[n, xl] += pr[n % 2, xl]
        second[n] = [
            remote(acc.at[n, xr, hr:rows], r2.at[n, 0, hr:rows], to_r),
            remote(acc.at[n, xl, 0:hr], r2.at[n, 1, 0:hr], to_l),
        ]
        acc[n, x] += pr[n % 2, x]
        if n + 2 < CHUNKS:
            pl.semaphore_signal(credit.at[n % 2], inc=1, device_id=to_p, device_id_type=MESH)

    def phase_c(n):
        first[n][0].wait_recv()
        acc[n, xr, 0:hr] += r1[n, 0]
        second[n].append(remote(acc.at[n, xr, 0:hr], r2.at[n, 0, 0:hr], to_r))
        first[n][1].wait_recv()
        acc[n, xl, hr:rows] += r1[n, 1]
        second[n].append(remote(acc.at[n, xl, hr:rows], r2.at[n, 1, hr:rows], to_l))

    def place(n, quarter, lo, hi):
        return out.at[pl.ds(pl.multiple_of(quarter * rows + lo, hr), hi - lo), n * cw:(n + 1) * cw]

    def phase_d(n):
        arrive(second[n])
        fin[n] = (acc[n, x] + r2[n, 0] + r2[n, 1]).astype(jnp.bfloat16)
        outs[n] = [remote(fin.at[n], place(n, q, 0, rows), dev) for dev in (up_r, up_l)]
        locals_.append(local(fin.at[n], place(n, q, 0, rows)))

    def phase_e(n):
        arrive(outs[n])
        fouts[n] = [
            remote(place(n, yl, 0, hr), place(n, yl, 0, hr), up_r),
            remote(place(n, yr, hr, rows), place(n, yr, hr, rows), up_l),
        ]

    phase_a(0)
    phase_b(0)
    fdn[2] = pass_dn(2, dn[2])
    phase_a(1)
    phase_b(1)
    phase_c(0)
    fdn[3] = pass_dn(3, dn[3])
    phase_a(2)
    phase_b(2)
    phase_c(1)
    phase_d(0)
    phase_a(3)
    phase_b(3)
    phase_c(2)
    phase_d(1)
    phase_e(0)
    phase_c(3)
    phase_d(2)
    phase_e(1)
    phase_d(3)
    phase_e(2)
    phase_e(3)
    for n in range(CHUNKS):
        arrive(fouts[n])
    for cp in sends:
        cp.wait_send()
    for cp in locals_:
        cp.wait()


def solution(mesh):
    row_spec = P(('dp', 'ep'), None)
    col_spec = P('ep', None, 'etp')
    in_specs = (row_spec, row_spec, row_spec, row_spec, col_spec, col_spec, P('ep', 'etp', None))
    n_q = mesh.shape['etp']
    group = mesh.shape['ep']

    def device_step(hidden, expert_ids, gate_wts, slot_pos, w_gate, w_up, w_down):
        rows_dev, d_model = hidden.shape
        n_e, _, width = w_gate.shape
        rows = rows_dev // n_q
        cw = d_model // CHUNKS
        nx = group // 2
        start = lax.axis_index('etp') * rows
        cut = lambda a: lax.dynamic_slice_in_dim(a, start, rows, axis=0).T
        ids, gts, pos = cut(expert_ids), cut(gate_wts), cut(slot_pos)
        wanted = jnp.arange(group, dtype=jnp.int32)[:, None] * n_e + jnp.arange(8, dtype=jnp.int32)[None, :]
        wanted = jnp.where(jnp.arange(8)[None, :] < n_e, wanted, -1)
        hit = (ids[None, None] == wanted[:, :, None, None]) & (pos >= 0)[None, None]
        dense = jnp.sum(jnp.where(hit, gts[None, None], 0.0), axis=2)
        f32, bf16 = jnp.float32, jnp.bfloat16
        return pl.pallas_call(
            functools.partial(moe_kernel, n_q, group),
            out_shape=jax.ShapeDtypeStruct((rows_dev, d_model), bf16),
            in_specs=[pl.BlockSpec(memory_space=pl.ANY)] * 5,
            out_specs=pl.BlockSpec(memory_space=pl.ANY),
            scratch_shapes=[
                pltpu.VMEM((group, rows, d_model), bf16),
                pltpu.VMEM((group, group, 8, rows), f32),
                pltpu.VMEM((n_e, n_q, d_model, 2 * width), bf16),
                pltpu.VMEM((CHUNKS, n_e, n_q, width, cw), bf16),
                pltpu.VMEM((group * n_e, rows, n_q * width), bf16),
                pltpu.VMEM((nx, rows, cw), f32),
                pltpu.VMEM((2, nx, rows, cw), f32),
                pltpu.VMEM((CHUNKS, nx, rows, cw), f32),
                pltpu.VMEM((CHUNKS, 2, rows // 2, cw), f32),
                pltpu.VMEM((CHUNKS, 2, rows, cw), f32),
                pltpu.VMEM((CHUNKS, rows, cw), bf16),
                pltpu.SemaphoreType.DMA((104,)),
                pltpu.SemaphoreType.DMA((104,)),
                pltpu.SemaphoreType.DMA((20,)),
                pltpu.SemaphoreType.REGULAR((2,)),
            ],
            compiler_params=pltpu.CompilerParams(collective_id=0, has_side_effects=True, vmem_limit_bytes=67043328),
        )(hidden, dense, w_gate, w_up, w_down)

    return jax.shard_map(device_step, mesh=mesh, in_specs=in_specs, out_specs=row_spec, check_vma=False)
```

```python
import functools

import jax
import jax.numpy as jnp
from jax import lax
from jax.experimental import pallas as pl
from jax.experimental.pallas import tpu as pltpu
from jax.sharding import PartitionSpec as P

MESH = pl.DeviceIdType.MESH
EIGHTHS = (2, 2, 2, 1, 1)


def moe_kernel(n_q, group, hid, ids, gts, pos, wg, wu, wd, out, tok, ids_v, gts_v, pos_v, gcol, wgu, act, spart, pr, *rest):
    n_c = len(EIGHTHS)
    wdn, acc, r1, r2, fin = (rest[i * n_c:(i + 1) * n_c] for i in range(5))
    ssem, rsem, lsem, credit = rest[5 * n_c:]
    rows, d_model = tok.shape[1:]
    n_e, width = wg.shape[0], wg.shape[2]
    nx = group // 2
    hr, hk, he = rows // 2, d_model // 2, n_e // 2
    wide = [k * (d_model // 8) for k in EIGHTHS]
    cols = [slice(sum(wide[:n]), sum(wide[:n + 1])) for n in range(n_c)]
    q, ep = lax.axis_index('etp'), lax.axis_index('ep')
    x, c = lax.div(ep, 2), lax.rem(ep, 2)
    yl, yr = lax.rem(q + n_q - 1, n_q), lax.rem(q + 1, n_q)
    xl, xr, xf = lax.rem(x + nx - 1, nx), lax.rem(x + 1, nx), lax.rem(x + 2, nx)
    bl, br, bf = xl * 2 + c, xr * 2 + c, xf * 2 + c
    to_l, to_r, to_p = {'ep': bl}, {'ep': br}, {'ep': x * 2 + 1 - c}
    up_l, up_r = {'etp': yl}, {'etp': yr}
    used = [0, 0]
    sends, placed = [], []

    def remote(src, dst, dev):
        k = used[0]
        used[0] += 1
        cp = pltpu.make_async_remote_copy(src_ref=src, dst_ref=dst, send_sem=ssem.at[k], recv_sem=rsem.at[k], device_id=dev, device_id_type=MESH)
        cp.start()
        sends.append(cp)
        return cp

    def local(src, dst):
        k = used[1]
        used[1] += 1
        cp = pltpu.make_async_copy(src, dst, lsem.at[k])
        cp.start()
        return cp

    def arrive(cps):
        for cp in cps:
            cp.wait_recv()

    barrier = pltpu.get_barrier_semaphore()
    for dev in (to_l, to_r, to_p, up_l, up_r):
        pl.semaphore_signal(barrier, inc=1, device_id=dev, device_id_type=MESH)
    pl.semaphore_wait(barrier, 5)

    def send_gu(e):
        cps = []
        for slot, dev in ((1, up_r), (2, up_l)):
            cps.append(remote(wg.at[e], wgu.at[e, slot, :, 0:width], dev))
            cps.append(remote(wu.at[e], wgu.at[e, slot, :, width:2 * width], dev))
        return cps

    def pass_gu(e, cps):
        arrive(cps)
        return [
            remote(wgu.at[e, 1, 0:hk], wgu.at[e, 3, 0:hk], up_r),
            remote(wgu.at[e, 2, hk:d_model], wgu.at[e, 3, hk:d_model], up_l),
        ]

    def send_dn(n):
        return [remote(wd.at[:, :, cols[n]], wdn[n].at[:, slot], dev) for slot, dev in ((1, up_r), (2, up_l))]

    def pass_dn(n, cps):
        arrive(cps)
        return [
            remote(wdn[n].at[0:he, 1], wdn[n].at[0:he, 3], up_r),
            remote(wdn[n].at[he:n_e, 2], wdn[n].at[he:n_e, 3], up_l),
        ]

    start = pl.multiple_of(q * rows, rows)
    own_rows = hid.at[pl.ds(start, rows)]
    route = [(a.at[:, pl.ds(start, rows)], v) for a, v in ((ids, ids_v), (gts, gts_v), (pos, pos_v))]

    def send_tok(dev):
        return [remote(own_rows, tok.at[ep], dev)] + [remote(a, v.at[ep], dev) for a, v in route]

    def pass_route(b, dev):
        return [remote(v.at[b], v.at[b], dev) for v in (ids_v, gts_v, pos_v)]

    gu = {0: send_gu(0)}
    tok_p, tok_r, tok_l = send_tok(to_p), send_tok(to_r), send_tok(to_l)
    gu[1] = send_gu(1)
    mine = [local(own_rows, tok.at[ep])] + [local(a, v.at[ep]) for a, v in route]
    for e in range(n_e):
        mine.append(local(wg.at[e], wgu.at[e, 0, :, 0:width]))
        mine.append(local(wu.at[e], wgu.at[e, 0, :, width:2 * width]))
    for n in range(n_c):
        mine.append(local(wd.at[:, :, cols[n]], wdn[n].at[:, 0]))

    def block_at(o):
        h = lax.div(o, 2)
        xi = lax.rem(x + h + lax.div(h, 2) - 2 * lax.div(h, 3), nx)
        return xi * 2 + lax.rem(o, 2)

    def make_gates(lo, hi):
        def body(o, carry):
            b = block_at(o)
            weight = jnp.where(pos_v[b] >= 0, gts_v[b], 0.0)
            chosen = ids_v[b]
            line = lax.broadcasted_iota(jnp.int32, weight.shape, 0)
            table = jnp.zeros_like(weight)
            for e in range(n_e):
                one = jnp.sum(jnp.where(chosen == ep * n_e + e, weight, 0.0), axis=0, keepdims=True)
                table = jnp.where(line == e, one, table)
            gcol[b] = table.T
            return carry

        lax.fori_loop(lo, hi, body, 0)

    def up(e0, e1, slots, lo, hi):
        def body(t, carry):
            b = block_at(lo + lax.div(t, e1 - e0))
            e = e0 + lax.rem(t, e1 - e0)
            gate = gcol[b, :, e0:e0 + 1] if e1 - e0 == 1 else None
            if gate is None:
                lane = lax.broadcasted_iota(jnp.int32, gcol.shape[1:], 1)
                gate = jnp.sum(jnp.where(lane == e, gcol[b], 0.0), axis=1, keepdims=True)
            for s in slots:
                prod = jnp.dot(tok[b], wgu[e, s], preferred_element_type=jnp.float32)
                h = jnp.where(gate > 0, jax.nn.silu(prod[:, :width]) * prod[:, width:], 0.0)
                act[b * n_e + e, :, s * width:(s + 1) * width] = h.astype(jnp.bfloat16)
            return carry

        lax.fori_loop(0, (hi - lo) * (e1 - e0), body, 0)

    fwd, dn, fdn = {}, {}, {}
    for cp in mine:
        cp.wait()
    arrive(tok_p)
    make_gates(0, 2)
    up(0, n_e, (0,), 0, 2)
    fwd[0] = pass_gu(0, gu[0])
    gu[2] = send_gu(2)
    up(0, 1, (1, 2), 0, 2)
    fwd[1] = pass_gu(1, gu[1])
    gu[3] = send_gu(3)
    up(1, 2, (1, 2), 0, 2)
    arrive(tok_r)
    arrive(tok_l)
    relay = [remote(tok.at[b], tok.at[b], to_p) for b in (bl, br)]
    far = [
        remote(tok.at[bl, 0:hr], tok.at[bl, 0:hr], to_r),
        remote(tok.at[br, hr:rows], tok.at[br, hr:rows], to_l),
    ]
    relay += pass_route(bl, to_p) + pass_route(br, to_p)
    far += pass_route(bl, to_r)
    arrive(relay)
    make_gates(2, 6)
    up(0, n_e, (0,), 2, 6)
    up(0, 2, (1, 2), 2, 6)
    arrive(far)
    relay = [remote(tok.at[bf], tok.at[bf], to_p)] + pass_route(bf, to_p)
    arrive(fwd[0])
    up(0, 1, (3,), 0, 6)
    fwd[2] = pass_gu(2, gu[2])
    arrive(relay)
    make_gates(6, 8)
    up(0, n_e, (0,), 6, 8)
    up(0, 2, (1, 2), 6, 8)
    up(0, 1, (3,), 6, 8)
    up(2, 3, (1, 2), 0, 8)
    arrive(fwd[1])
    up(1, 2, (3,), 0, 8)
    fwd[3] = pass_gu(3, gu[3])
    dn[0] = send_dn(0)
    up(3, 4, (1, 2), 0, 8)
    arrive(fwd[2])
    up(2, 3, (3,), 0, 8)
    arrive(fwd[3])
    up(3, 4, (3,), 0, 8)

    def down(n, b, dst):
        for e in range(n_e):
            mat = wdn[n][e].reshape(n_q * width, wide[n])
            term = gcol[b, :, e:e + 1] * jnp.dot(act[b * n_e + e], mat, preferred_element_type=jnp.float32)
            if e == 0:
                dst[...] = term
            else:
                dst[...] += term

    d2d, first, second, outs, fouts = {}, {}, {}, {}, {}

    def phase_a(n):
        arrive(fdn[n])
        if n >= 1:
            d2d[n - 1].wait_send()
            sends[:] = [cp for cp in sends if cp is not d2d[n - 1]]
        half = spart.at[:, :, 0:wide[n]]

        def other(i, carry):
            xi = lax.rem(xf + i, nx)
            down(n, xi * 2 + 1 - c, half.at[xi])
            return carry

        lax.fori_loop(0, nx, other, 0)
        if n >= 2:
            pl.semaphore_wait(credit.at[n % 2], 1)
        d2d[n] = remote(half, pr.at[n % 2, :, :, 0:wide[n]], to_p)

        def own(i, carry):
            xi = lax.rem(xf + i, nx)
            down(n, xi * 2 + c, acc[n].at[xi])
            return carry

        lax.fori_loop(0, nx, own, 0)

    def phase_b(n):
        d2d[n].wait_recv()

        def join(xi):
            acc[n][xi] += pr[n % 2, xi, :, 0:wide[n]]

        join(xf)
        first[n] = [
            remote(acc[n].at[xf, 0:hr], r1[n].at[0], to_r),
            remote(acc[n].at[xf, hr:rows], r1[n].at[1], to_l),
        ]
        join(xr)
        join(xl)
        second[n] = [
            remote(acc[n].at[xr, hr:rows], r2[n].at[0, hr:rows], to_r),
            remote(acc[n].at[xl, 0:hr], r2[n].at[1, 0:hr], to_l),
        ]
        join(x)
        if n + 2 < n_c:
            pl.semaphore_signal(credit.at[n % 2], inc=1, device_id=to_p, device_id_type=MESH)

    def phase_c(n):
        first[n][0].wait_recv()
        acc[n][xr, 0:hr] += r1[n][0]
        second[n].append(remote(acc[n].at[xr, 0:hr], r2[n].at[0, 0:hr], to_r))
        first[n][1].wait_recv()
        acc[n][xl, hr:rows] += r1[n][1]
        second[n].append(remote(acc[n].at[xl, hr:rows], r2[n].at[1, hr:rows], to_l))

    def place(n, quarter, lo, hi):
        return out.at[pl.ds(pl.multiple_of(quarter * rows + lo, hr), hi - lo), cols[n]]

    def phase_d(n):
        arrive(second[n])
        fin[n][...] = (acc[n][x] + r2[n][0] + r2[n][1]).astype(jnp.bfloat16)
        outs[n] = [remote(fin[n], place(n, q, 0, rows), dev) for dev in (up_r, up_l)]
        placed.append(local(fin[n], place(n, q, 0, rows)))

    def phase_e(n):
        arrive(outs[n])
        fouts[n] = [
            remote(place(n, yl, 0, hr), place(n, yl, 0, hr), up_r),
            remote(place(n, yr, hr, rows), place(n, yr, hr, rows), up_l),
        ]

    fdn[0] = pass_dn(0, dn[0])
    dn[1] = send_dn(1)
    dn[2] = send_dn(2)
    phase_a(0)
    phase_b(0)
    fdn[1] = pass_dn(1, dn[1])
    dn[3] = send_dn(3)
    dn[4] = send_dn(4)
    phase_c(0)
    phase_a(1)
    phase_b(1)
    fdn[2] = pass_dn(2, dn[2])
    phase_a(2)
    phase_b(2)
    fdn[3] = pass_dn(3, dn[3])
    phase_c(1)
    phase_d(0)
    phase_a(3)
    phase_b(3)
    fdn[4] = pass_dn(4, dn[4])
    phase_c(2)
    phase_d(1)
    phase_e(0)
    phase_a(4)
    phase_b(4)
    phase_c(3)
    phase_d(2)
    phase_e(1)
    phase_c(4)
    phase_d(3)
    phase_e(2)
    phase_d(4)
    phase_e(3)
    phase_e(4)
    for n in range(n_c):
        arrive(fouts[n])
    for cp in sends:
        cp.wait_send()
    for cp in placed:
        cp.wait()


def solution(mesh):
    row_spec = P(('dp', 'ep'), None)
    col_spec = P('ep', None, 'etp')
    in_specs = (row_spec, row_spec, row_spec, row_spec, col_spec, col_spec, P('ep', 'etp', None))
    n_q = mesh.shape['etp']
    group = mesh.shape['ep']

    def device_step(hidden, expert_ids, gate_wts, slot_pos, w_gate, w_up, w_down):
        rows_dev, d_model = hidden.shape
        top_k = expert_ids.shape[1]
        n_e, _, width = w_gate.shape
        rows = rows_dev // n_q
        nx = group // 2
        f32, bf16, i32 = jnp.float32, jnp.bfloat16, jnp.int32
        wide = [k * (d_model // 8) for k in EIGHTHS]
        chunked = [pltpu.VMEM((n_e, n_q, width, w), bf16) for w in wide]
        chunked += [pltpu.VMEM((nx, rows, w), f32) for w in wide]
        chunked += [pltpu.VMEM((2, rows // 2, w), f32) for w in wide]
        chunked += [pltpu.VMEM((2, rows, w), f32) for w in wide]
        chunked += [pltpu.VMEM((rows, w), bf16) for w in wide]
        return pl.pallas_call(
            functools.partial(moe_kernel, n_q, group),
            out_shape=jax.ShapeDtypeStruct((rows_dev, d_model), bf16),
            in_specs=[pl.BlockSpec(memory_space=pl.ANY)] * 7,
            out_specs=pl.BlockSpec(memory_space=pl.ANY),
            scratch_shapes=[
                pltpu.VMEM((group, rows, d_model), bf16),
                pltpu.VMEM((group, top_k, rows), i32),
                pltpu.VMEM((group, top_k, rows), f32),
                pltpu.VMEM((group, top_k, rows), i32),
                pltpu.VMEM((group, rows, top_k), f32),
                pltpu.VMEM((n_e, n_q, d_model, 2 * width), bf16),
                pltpu.VMEM((group * n_e, rows, n_q * width), bf16),
                pltpu.VMEM((nx, rows, max(wide)), f32),
                pltpu.VMEM((2, nx, rows, max(wide)), f32),
                *chunked,
                pltpu.SemaphoreType.DMA((132,)),
                pltpu.SemaphoreType.DMA((132,)),
                pltpu.SemaphoreType.DMA((24,)),
                pltpu.SemaphoreType.REGULAR((2,)),
            ],
            compiler_params=pltpu.CompilerParams(collective_id=0, has_side_effects=True, vmem_limit_bytes=67043328),
        )(hidden, expert_ids.T, gate_wts.T, slot_pos.T, w_gate, w_up, w_down)

    return jax.shard_map(device_step, mesh=mesh, in_specs=in_specs, out_specs=row_spec, check_vma=False)
```

```python
import functools

import jax
import jax.numpy as jnp
from jax import lax
from jax.experimental import pallas as pl
from jax.experimental.pallas import tpu as pltpu
from jax.sharding import PartitionSpec as P

MESH = pl.DeviceIdType.MESH
EIGHTHS = (1, 2, 2, 2, 1)


def moe_kernel(n_q, group, hid, ids, gts, pos, wg, wu, wd, out, tok, ids_v, gts_v, pos_v, gcol, wgu, act, spart, pr, *rest):
    n_c = len(EIGHTHS)
    wdn, acc, r1, r2 = (list(rest[i * n_c:(i + 1) * n_c]) for i in range(4))
    ssem, rsem, lsem, credit = rest[4 * n_c:]
    rows, d_model = tok.shape[1:]
    n_e, width = wg.shape[0], wg.shape[2]
    nx = group // 2
    hr, hk, he = rows // 2, d_model // 2, n_e // 2
    acc[n_c - 1] = acc[0]
    wide = [k * (d_model // 8) for k in EIGHTHS]
    cols = [slice(sum(wide[:n]), sum(wide[:n + 1])) for n in range(n_c)]
    q, ep = lax.axis_index('etp'), lax.axis_index('ep')
    x, c = lax.div(ep, 2), lax.rem(ep, 2)
    yl, yr = lax.rem(q + n_q - 1, n_q), lax.rem(q + 1, n_q)
    xl, xr, xf = lax.rem(x + nx - 1, nx), lax.rem(x + 1, nx), lax.rem(x + 2, nx)
    bl, br, bf = xl * 2 + c, xr * 2 + c, xf * 2 + c
    to_l, to_r, to_p = {'ep': bl}, {'ep': br}, {'ep': x * 2 + 1 - c}
    up_l, up_r = {'etp': yl}, {'etp': yr}
    used = [0, 0]
    sends = []

    def remote(src, dst, dev):
        k = used[0]
        used[0] += 1
        cp = pltpu.make_async_remote_copy(src_ref=src, dst_ref=dst, send_sem=ssem.at[k], recv_sem=rsem.at[k], device_id=dev, device_id_type=MESH)
        cp.start()
        sends.append(cp)
        return cp

    def local(src, dst):
        k = used[1]
        used[1] += 1
        cp = pltpu.make_async_copy(src, dst, lsem.at[k])
        cp.start()
        return cp

    def arrive(cps):
        for cp in cps:
            cp.wait_recv()

    barrier = pltpu.get_barrier_semaphore()
    for dev in (to_l, to_r, to_p, up_l, up_r):
        pl.semaphore_signal(barrier, inc=1, device_id=dev, device_id_type=MESH)

    start = pl.multiple_of(q * rows, rows)
    route = [(a.at[:, pl.ds(start, rows)], v) for a, v in ((ids, ids_v), (gts, gts_v), (pos, pos_v))]

    def load_gu(e):
        return [local(wg.at[e], wgu.at[e, 0, :, 0:width]), local(wu.at[e], wgu.at[e, 0, :, width:2 * width])]

    mine_gu = {0: load_gu(0)}
    mine_tok = [local(hid.at[pl.ds(start, rows)], tok.at[ep])] + [local(a, v.at[ep]) for a, v in route]
    for e in range(1, n_e):
        mine_gu[e] = load_gu(e)
    mine_dn = [local(wd.at[:, :, cols[n]], wdn[n].at[:, 0]) for n in range(n_c)]
    pl.semaphore_wait(barrier, 5)

    def send_gu(e):
        if e < 2:
            for cp in mine_gu[e]:
                cp.wait()
        return [remote(wgu.at[e, 0], wgu.at[e, slot], dev) for slot, dev in ((1, up_r), (2, up_l))]

    def pass_gu(e, cps):
        arrive(cps)
        return [
            remote(wgu.at[e, 1, 0:hk], wgu.at[e, 3, 0:hk], up_r),
            remote(wgu.at[e, 2, hk:d_model], wgu.at[e, 3, hk:d_model], up_l),
        ]

    def send_dn(n):
        mine_dn[n].wait()
        return [remote(wdn[n].at[:, 0], wdn[n].at[:, slot], dev) for slot, dev in ((1, up_r), (2, up_l))]

    def pass_dn(n, cps):
        arrive(cps)
        return [
            remote(wdn[n].at[0:he, 1], wdn[n].at[0:he, 3], up_r),
            remote(wdn[n].at[he:n_e, 2], wdn[n].at[he:n_e, 3], up_l),
        ]

    def send_tok(dev):
        return [remote(tok.at[ep], tok.at[ep], dev)] + pass_route(ep, dev)

    def pass_route(b, dev):
        return [remote(v.at[b], v.at[b], dev) for v in (ids_v, gts_v, pos_v)]

    gu = {0: send_gu(0)}
    for cp in mine_tok:
        cp.wait()
    tok_r, tok_l, tok_p = send_tok(to_r), send_tok(to_l), send_tok(to_p)
    gu[1] = send_gu(1)

    def block_at(o):
        h = lax.div(o, 2)
        xi = lax.rem(x + h + lax.div(h, 2) - 2 * lax.div(h, 3), nx)
        return xi * 2 + lax.rem(o, 2)

    def make_gates(lo, hi):
        def body(o, carry):
            b = block_at(o)
            weight = jnp.where(pos_v[b] >= 0, gts_v[b], 0.0)
            chosen = ids_v[b]
            line = lax.broadcasted_iota(jnp.int32, weight.shape, 0)
            table = jnp.zeros_like(weight)
            for e in range(n_e):
                one = jnp.sum(jnp.where(chosen == ep * n_e + e, weight, 0.0), axis=0, keepdims=True)
                table = jnp.where(line == e, one, table)
            gcol[b] = table.T
            return carry

        lax.fori_loop(lo, hi, body, 0)

    def up(e0, e1, slots, lo, hi):
        span = e1 - e0
        total = (hi - lo) * span
        step = max(span, 4 // len(slots))
        while total % step:
            step -= 1

        def body(i, carry):
            for k in range(step):
                b, e = block_at(lo + i * (step // span) + k // span), e0 + k % span
                gate = gcol[b, :, e:e + 1]
                for s in slots:
                    prod = jnp.dot(tok[b], wgu[e, s], preferred_element_type=jnp.float32)
                    h = jnp.where(gate > 0, jax.nn.silu(prod[:, :width]) * prod[:, width:], 0.0)
                    act[b * n_e + e, :, s * width:(s + 1) * width] = h.astype(jnp.bfloat16)
            return carry

        lax.fori_loop(0, total // step, body, 0)

    fwd, dn, fdn = {}, {}, {}
    for e in range(2, n_e):
        for cp in mine_gu[e]:
            cp.wait()
    arrive(tok_p)
    make_gates(0, 2)
    up(0, n_e, (0,), 0, 2)
    fwd[0] = pass_gu(0, gu[0])
    gu[2] = send_gu(2)
    up(0, 1, (1, 2), 0, 2)
    fwd[1] = pass_gu(1, gu[1])
    gu[3] = send_gu(3)
    up(1, 2, (1, 2), 0, 2)
    arrive(tok_r)
    arrive(tok_l)
    relay = [remote(tok.at[b], tok.at[b], to_p) for b in (bl, br)]
    far = [
        remote(tok.at[bl, 0:hr], tok.at[bl, 0:hr], to_r),
        remote(tok.at[br, hr:rows], tok.at[br, hr:rows], to_l),
    ]
    relay += pass_route(bl, to_p) + pass_route(br, to_p)
    far += pass_route(bl, to_r)
    arrive(relay)
    make_gates(2, 6)
    up(0, n_e, (0,), 2, 6)
    up(0, 2, (1, 2), 2, 6)
    arrive(far)
    relay = [remote(tok.at[bf], tok.at[bf], to_p)] + pass_route(bf, to_p)
    arrive(fwd[0])
    up(0, 1, (3,), 0, 6)
    fwd[2] = pass_gu(2, gu[2])
    arrive(relay)
    make_gates(6, 8)
    up(0, n_e, (0,), 6, 8)
    up(0, 2, (1, 2), 6, 8)
    up(0, 1, (3,), 6, 8)
    up(2, 3, (1, 2), 0, 8)
    arrive(fwd[1])
    up(1, 2, (3,), 0, 8)
    fwd[3] = pass_gu(3, gu[3])
    dn[0] = send_dn(0)
    up(3, 4, (1, 2), 0, 8)
    arrive(fwd[2])
    up(2, 3, (3,), 0, 8)
    arrive(fwd[3])
    up(3, 4, (3,), 0, 8)

    def down(n, b, dst):
        for e in range(n_e):
            mat = wdn[n][e].reshape(n_q * width, wide[n])
            term = gcol[b, :, e:e + 1] * jnp.dot(act[b * n_e + e], mat, preferred_element_type=jnp.float32)
            if e == 0:
                dst[...] = term
            else:
                dst[...] += term

    d2d, first, second, outs, fouts = {}, {}, {}, {}, {}

    def phase_a(n):
        arrive(fdn[n])
        if n >= 1:
            d2d[n - 1].wait_send()
            sends[:] = [cp for cp in sends if cp is not d2d[n - 1]]
        if n == n_c - 1:
            drained = first[0] + second[0]
            for cp in drained:
                cp.wait_send()
            sends[:] = [cp for cp in sends if not any(cp is old for old in drained)]
        half = spart.at[:, :, 0:wide[n]]

        def other(i, carry):
            xi = lax.rem(xf + i, nx)
            down(n, xi * 2 + 1 - c, half.at[xi])
            return carry

        lax.fori_loop(0, nx, other, 0)
        if n >= 2:
            pl.semaphore_wait(credit.at[n % 2], 1)
        d2d[n] = remote(half, pr.at[n % 2, :, :, 0:wide[n]], to_p)

        def own(i, carry):
            xi = lax.rem(xf + i, nx)
            down(n, xi * 2 + c, acc[n].at[xi])
            return carry

        lax.fori_loop(0, nx, own, 0)

    def phase_b(n):
        d2d[n].wait_recv()

        def join(xi):
            acc[n][xi] += pr[n % 2, xi, :, 0:wide[n]]

        join(xf)
        first[n] = [
            remote(acc[n].at[xf, 0:hr], r1[n].at[0], to_r),
            remote(acc[n].at[xf, hr:rows], r1[n].at[1], to_l),
        ]
        join(xr)
        join(xl)
        second[n] = [
            remote(acc[n].at[xr, hr:rows], r2[n].at[0, hr:rows], to_r),
            remote(acc[n].at[xl, 0:hr], r2[n].at[1, 0:hr], to_l),
        ]
        join(x)
        if n + 2 < n_c:
            pl.semaphore_signal(credit.at[n % 2], inc=1, device_id=to_p, device_id_type=MESH)

    def phase_c(n):
        first[n][0].wait_recv()
        acc[n][xr, 0:hr] += r1[n][0]
        second[n].append(remote(acc[n].at[xr, 0:hr], r2[n].at[0, 0:hr], to_r))
        first[n][1].wait_recv()
        acc[n][xl, hr:rows] += r1[n][1]
        second[n].append(remote(acc[n].at[xl, hr:rows], r2[n].at[1, hr:rows], to_l))

    def place(n, quarter, lo, hi):
        return out.at[pl.ds(pl.multiple_of(quarter * rows + lo, hr), hi - lo), cols[n]]

    def phase_d(n):
        arrive(second[n])
        total = acc[n][x] + r2[n][0] + r2[n][1]
        out[pl.ds(start, rows), cols[n]] = total.astype(jnp.bfloat16)
        outs[n] = [remote(place(n, q, 0, rows), place(n, q, 0, rows), dev) for dev in (up_r, up_l)]

    def phase_e(n):
        arrive(outs[n])
        fouts[n] = [
            remote(place(n, yl, 0, hr), place(n, yl, 0, hr), up_r),
            remote(place(n, yr, hr, rows), place(n, yr, hr, rows), up_l),
        ]

    fdn[0] = pass_dn(0, dn[0])
    dn[1] = send_dn(1)
    dn[2] = send_dn(2)
    phase_a(0)
    phase_b(0)
    fdn[1] = pass_dn(1, dn[1])
    dn[3] = send_dn(3)
    dn[4] = send_dn(4)
    phase_c(0)
    phase_a(1)
    phase_b(1)
    fdn[2] = pass_dn(2, dn[2])
    phase_a(2)
    phase_b(2)
    fdn[3] = pass_dn(3, dn[3])
    phase_c(1)
    phase_d(0)
    phase_a(3)
    phase_b(3)
    fdn[4] = pass_dn(4, dn[4])
    phase_c(2)
    phase_d(1)
    phase_e(0)
    phase_a(4)
    phase_b(4)
    phase_c(3)
    phase_d(2)
    phase_e(1)
    phase_c(4)
    phase_d(3)
    phase_e(2)
    phase_d(4)
    phase_e(3)
    phase_e(4)
    for n in range(n_c):
        arrive(fouts[n])
    for cp in sends:
        cp.wait_send()


def solution(mesh):
    row_spec = P(('dp', 'ep'), None)
    col_spec = P('ep', None, 'etp')
    in_specs = (row_spec, row_spec, row_spec, row_spec, col_spec, col_spec, P('ep', 'etp', None))
    n_q = mesh.shape['etp']
    group = mesh.shape['ep']

    def device_step(hidden, expert_ids, gate_wts, slot_pos, w_gate, w_up, w_down):
        rows_dev, d_model = hidden.shape
        top_k = expert_ids.shape[1]
        n_e, _, width = w_gate.shape
        rows = rows_dev // n_q
        nx = group // 2
        f32, bf16, i32 = jnp.float32, jnp.bfloat16, jnp.int32
        wide = [k * (d_model // 8) for k in EIGHTHS]
        chunked = [pltpu.VMEM((n_e, n_q, width, w), bf16) for w in wide]
        chunked += [pltpu.VMEM((nx, rows, w) if n < len(wide) - 1 else (8, 128), f32) for n, w in enumerate(wide)]
        chunked += [pltpu.VMEM((2, rows // 2, w), f32) for w in wide]
        chunked += [pltpu.VMEM((2, rows, w), f32) for w in wide]
        return pl.pallas_call(
            functools.partial(moe_kernel, n_q, group),
            out_shape=pltpu.VMEM((rows_dev, d_model), bf16),
            in_specs=[pl.BlockSpec(memory_space=pl.ANY)] * 7,
            out_specs=pl.BlockSpec(memory_space=pltpu.VMEM),
            scratch_shapes=[
                pltpu.VMEM((group, rows, d_model), bf16),
                pltpu.VMEM((group, top_k, rows), i32),
                pltpu.VMEM((group, top_k, rows), f32),
                pltpu.VMEM((group, top_k, rows), i32),
                pltpu.VMEM((group, rows, top_k), f32),
                pltpu.VMEM((n_e, n_q, d_model, 2 * width), bf16),
                pltpu.VMEM((group * n_e, rows, n_q * width), bf16),
                pltpu.VMEM((nx, rows, max(wide)), f32),
                pltpu.VMEM((2, nx, rows, max(wide)), f32),
                *chunked,
                pltpu.SemaphoreType.DMA((132,)),
                pltpu.SemaphoreType.DMA((132,)),
                pltpu.SemaphoreType.DMA((24,)),
                pltpu.SemaphoreType.REGULAR((2,)),
            ],
            compiler_params=pltpu.CompilerParams(collective_id=0, has_side_effects=True, vmem_limit_bytes=59 * 1024 * 1024),
        )(hidden, expert_ids.T, gate_wts.T, slot_pos.T, w_gate, w_up, w_down)

    return jax.shard_map(device_step, mesh=mesh, in_specs=in_specs, out_specs=row_spec, check_vma=False)
```

```python
import functools

import jax
import jax.numpy as jnp
from jax import lax
from jax.experimental import pallas as pl
from jax.experimental.pallas import tpu as pltpu
from jax.sharding import PartitionSpec as P

MESH = pl.DeviceIdType.MESH
EIGHTHS = (2, 2, 2, 1, 1)


def moe_kernel(n_q, group, hid, ids, gts, pos, wg, wu, wd, out, tok, ids_v, gts_v, pos_v, gcol, wgu, act, spart, pr, *rest):
    n_c = len(EIGHTHS)
    wdn, acc, r1, r2 = (list(rest[i * n_c:(i + 1) * n_c]) for i in range(4))
    ssem, rsem, lsem, credit = rest[4 * n_c:]
    rows, d_model = tok.shape[1:]
    n_e, width = wg.shape[0], wg.shape[2]
    nx = group // 2
    hr, hk, he = rows // 2, d_model // 2, n_e // 2
    wide = [k * (d_model // 8) for k in EIGHTHS]
    acc[n_c - 1] = acc[0].at[:, :, 0:wide[-1]]
    cols = [slice(sum(wide[:n]), sum(wide[:n + 1])) for n in range(n_c)]
    q, ep = lax.axis_index('etp'), lax.axis_index('ep')
    x, c = lax.div(ep, 2), lax.rem(ep, 2)
    yl, yr = lax.rem(q + n_q - 1, n_q), lax.rem(q + 1, n_q)
    xl, xr, xf = lax.rem(x + nx - 1, nx), lax.rem(x + 1, nx), lax.rem(x + 2, nx)
    bl, br, bf = xl * 2 + c, xr * 2 + c, xf * 2 + c
    to_l, to_r, to_p = {'ep': bl}, {'ep': br}, {'ep': x * 2 + 1 - c}
    up_l, up_r = {'etp': yl}, {'etp': yr}
    used = [0, 0]
    sends = []

    def remote(src, dst, dev):
        k = used[0]
        used[0] += 1
        cp = pltpu.make_async_remote_copy(src_ref=src, dst_ref=dst, send_sem=ssem.at[k], recv_sem=rsem.at[k], device_id=dev, device_id_type=MESH)
        cp.start()
        sends.append(cp)
        return cp

    def local(src, dst):
        k = used[1]
        used[1] += 1
        cp = pltpu.make_async_copy(src, dst, lsem.at[k])
        cp.start()
        return cp

    def arrive(cps):
        for cp in cps:
            cp.wait_recv()

    barrier = pltpu.get_barrier_semaphore()
    for dev in (to_l, to_r, to_p, up_l, up_r):
        pl.semaphore_signal(barrier, inc=1, device_id=dev, device_id_type=MESH)

    start = pl.multiple_of(q * rows, rows)
    route = [(a.at[:, pl.ds(start, rows)], v) for a, v in ((ids, ids_v), (gts, gts_v), (pos, pos_v))]

    def load_gu(e):
        return [local(wg.at[e], wgu.at[e, 0, :, 0:width]), local(wu.at[e], wgu.at[e, 0, :, width:2 * width])]

    mine_gu = {0: load_gu(0)}
    mine_tok = [local(hid.at[pl.ds(start, rows)], tok.at[ep])] + [local(a, v.at[ep]) for a, v in route]
    for e in range(1, n_e):
        mine_gu[e] = load_gu(e)
    mine_dn = [local(wd.at[:, :, cols[n]], wdn[n].at[:, 0]) for n in range(n_c)]
    pl.semaphore_wait(barrier, 5)

    def send_gu(e):
        if e < 2:
            for cp in mine_gu[e]:
                cp.wait()
        return [remote(wgu.at[e, 0], wgu.at[e, slot], dev) for slot, dev in ((1, up_r), (2, up_l))]

    def pass_gu(e, cps):
        arrive(cps)
        return [
            remote(wgu.at[e, 1, 0:hk], wgu.at[e, 3, 0:hk], up_r),
            remote(wgu.at[e, 2, hk:d_model], wgu.at[e, 3, hk:d_model], up_l),
        ]

    def send_dn(n):
        mine_dn[n].wait()
        return [remote(wdn[n].at[:, 0], wdn[n].at[:, slot], dev) for slot, dev in ((1, up_r), (2, up_l))]

    def pass_dn(n, cps):
        arrive(cps)
        return [
            remote(wdn[n].at[0:he, 1], wdn[n].at[0:he, 3], up_r),
            remote(wdn[n].at[he:n_e, 2], wdn[n].at[he:n_e, 3], up_l),
        ]

    def send_tok(dev):
        return [remote(tok.at[ep], tok.at[ep], dev)] + pass_route(ep, dev)

    def pass_route(b, dev):
        return [remote(v.at[b], v.at[b], dev) for v in (ids_v, gts_v, pos_v)]

    gu = {0: send_gu(0)}
    for cp in mine_tok:
        cp.wait()
    tok_r, tok_l, tok_p = send_tok(to_r), send_tok(to_l), send_tok(to_p)
    gu[1] = send_gu(1)

    def block_at(o):
        h = lax.div(o, 2)
        xi = lax.rem(x + h + lax.div(h, 2) - 2 * lax.div(h, 3), nx)
        return xi * 2 + lax.rem(o, 2)

    def make_gates(lo, hi):
        def body(o, carry):
            b = block_at(o)
            weight = jnp.where(pos_v[b] >= 0, gts_v[b], 0.0)
            chosen = ids_v[b]
            line = lax.broadcasted_iota(jnp.int32, weight.shape, 0)
            table = jnp.zeros_like(weight)
            for e in range(n_e):
                one = jnp.sum(jnp.where(chosen == ep * n_e + e, weight, 0.0), axis=0, keepdims=True)
                table = jnp.where(line == e, one, table)
            gcol[b] = table.T
            return carry

        lax.fori_loop(lo, hi, body, 0)

    def up(e0, e1, slots, lo, hi):
        span = e1 - e0
        total = (hi - lo) * span
        step = max(span, 4 // len(slots))
        while total % step:
            step -= 1

        def body(i, carry):
            for k in range(step):
                b, e = block_at(lo + i * (step // span) + k // span), e0 + k % span
                gate = gcol[b, :, e:e + 1]
                for s in slots:
                    prod = jnp.dot(tok[b], wgu[e, s], preferred_element_type=jnp.float32)
                    h = jnp.where(gate > 0, jax.nn.silu(prod[:, :width]) * prod[:, width:], 0.0)
                    act[b * n_e + e, :, s * width:(s + 1) * width] = h.astype(jnp.bfloat16)
            return carry

        lax.fori_loop(0, total // step, body, 0)

    fwd, dn, fdn = {}, {}, {}
    for e in range(2, n_e):
        for cp in mine_gu[e]:
            cp.wait()
    arrive(tok_p)
    make_gates(0, 2)
    up(0, n_e, (0,), 0, 2)
    fwd[0] = pass_gu(0, gu[0])
    gu[2] = send_gu(2)
    up(0, 1, (1, 2), 0, 2)
    fwd[1] = pass_gu(1, gu[1])
    gu[3] = send_gu(3)
    up(1, 2, (1, 2), 0, 2)
    arrive(tok_r)
    arrive(tok_l)
    relay = [remote(tok.at[b], tok.at[b], to_p) for b in (bl, br)]
    far = [
        remote(tok.at[bl, 0:hr], tok.at[bl, 0:hr], to_r),
        remote(tok.at[br, hr:rows], tok.at[br, hr:rows], to_l),
    ]
    relay += pass_route(bl, to_p) + pass_route(br, to_p)
    far += pass_route(bl, to_r)
    arrive(relay)
    make_gates(2, 6)
    up(0, n_e, (0,), 2, 6)
    up(0, 2, (1, 2), 2, 6)
    arrive(far)
    relay = [remote(tok.at[bf], tok.at[bf], to_p)] + pass_route(bf, to_p)
    arrive(fwd[0])
    up(0, 1, (3,), 0, 6)
    fwd[2] = pass_gu(2, gu[2])
    dn[0] = send_dn(0)
    arrive(relay)
    make_gates(6, 8)
    up(0, n_e, (0,), 6, 8)
    up(0, 2, (1, 2), 6, 8)
    up(0, 1, (3,), 6, 8)
    up(2, 3, (1, 2), 0, 8)
    arrive(fwd[1])
    up(1, 2, (3,), 0, 8)
    fwd[3] = pass_gu(3, gu[3])
    up(3, 4, (1, 2), 0, 8)
    arrive(fwd[2])
    up(2, 3, (3,), 0, 8)
    fdn[0] = pass_dn(0, dn[0])
    dn[1] = send_dn(1)
    arrive(fwd[3])
    up(3, 4, (3,), 0, 8)

    def down(n, b, dst):
        for e in range(n_e):
            mat = wdn[n][e].reshape(n_q * width, wide[n])
            term = gcol[b, :, e:e + 1] * jnp.dot(act[b * n_e + e], mat, preferred_element_type=jnp.float32)
            if e == 0:
                dst[...] = term
            else:
                dst[...] += term

    first, second, outs, fouts = {}, {}, {}, {}

    d2d_base, used[0] = used[0], used[0] + nx * n_c

    def to_partner(n, i):
        xi, k = lax.rem(xf + i, nx), d2d_base + n * nx + i
        return pltpu.make_async_remote_copy(
            src_ref=spart.at[xi, :, 0:wide[n]], dst_ref=pr.at[n % 2, xi, :, 0:wide[n]],
            send_sem=ssem.at[k], recv_sem=rsem.at[k], device_id=to_p, device_id_type=MESH)

    def products(n, lo, hi):
        def body(i, carry):
            xi = lax.rem(xf + i, nx)
            down(n, xi * 2 + 1 - c, spart.at[xi, :, 0:wide[n]])
            to_partner(n, i).start()
            down(n, xi * 2 + c, acc[n].at[xi])
            return carry

        lax.fori_loop(lo, hi, body, 0)

    def join(n, i):
        to_partner(n, i).wait_recv()
        xi = lax.rem(xf + i, nx)
        acc[n][xi] += pr[n % 2, xi, :, 0:wide[n]]

    def phase_ab(n):
        arrive(fdn[n])
        if n >= 1:
            for i in range(nx):
                to_partner(n - 1, i).wait_send()
        if n == n_c - 1:
            drained = first[0] + second[0]
            for cp in drained:
                cp.wait_send()
            sends[:] = [cp for cp in sends if not any(cp is old for old in drained)]
        if n >= 2:
            pl.semaphore_wait(credit.at[n % 2], 1)
        early = 2 if n == 0 else nx
        products(n, 0, early)
        join(n, 0)
        first[n] = [
            remote(acc[n].at[xf, 0:hr], r1[n].at[0], to_r),
            remote(acc[n].at[xf, hr:rows], r1[n].at[1], to_l),
        ]
        if early < nx:
            products(n, early, nx)
        join(n, 1)
        second[n] = [remote(acc[n].at[xl, 0:hr], r2[n].at[1, 0:hr], to_l)]
        join(n, 3)
        second[n].append(remote(acc[n].at[xr, hr:rows], r2[n].at[0, hr:rows], to_r))
        join(n, 2)
        if n + 2 < n_c:
            pl.semaphore_signal(credit.at[n % 2], inc=1, device_id=to_p, device_id_type=MESH)

    def phase_c(n):
        first[n][0].wait_recv()
        acc[n][xr, 0:hr] += r1[n][0]
        second[n].append(remote(acc[n].at[xr, 0:hr], r2[n].at[0, 0:hr], to_r))
        first[n][1].wait_recv()
        acc[n][xl, hr:rows] += r1[n][1]
        second[n].append(remote(acc[n].at[xl, hr:rows], r2[n].at[1, hr:rows], to_l))

    def place(n, quarter, lo, hi):
        return out.at[pl.ds(pl.multiple_of(quarter * rows + lo, hr), hi - lo), cols[n]]

    def phase_d(n):
        arrive(second[n])
        total = acc[n][x] + r2[n][0] + r2[n][1]
        out[pl.ds(start, rows), cols[n]] = total.astype(jnp.bfloat16)
        low, high = place(n, q, 0, hr), place(n, q, hr, rows)
        outs[n] = [remote(low, low, up_r), remote(high, high, up_l), remote(high, high, up_r), remote(low, low, up_l)]

    def phase_e(n):
        arrive(outs[n][:2])
        fouts[n] = [
            remote(place(n, yl, 0, hr), place(n, yl, 0, hr), up_r),
            remote(place(n, yr, hr, rows), place(n, yr, hr, rows), up_l),
        ]

    phase_ab(0)
    fdn[1] = pass_dn(1, dn[1])
    dn[2] = send_dn(2)
    phase_c(0)
    phase_ab(1)
    fdn[2] = pass_dn(2, dn[2])
    dn[3] = send_dn(3)
    dn[4] = send_dn(4)
    phase_ab(2)
    fdn[3] = pass_dn(3, dn[3])
    phase_c(1)
    phase_d(0)
    phase_ab(3)
    fdn[4] = pass_dn(4, dn[4])
    phase_c(2)
    phase_d(1)
    phase_e(0)
    phase_ab(4)
    phase_c(3)
    phase_d(2)
    phase_e(1)
    phase_c(4)
    phase_d(3)
    phase_e(2)
    phase_d(4)
    phase_e(3)
    phase_e(4)
    for i in range(nx):
        to_partner(n_c - 1, i).wait_send()
    for n in range(n_c):
        arrive(outs[n][2:] + fouts[n])
    for cp in sends:
        cp.wait_send()


def solution(mesh):
    row_spec = P(('dp', 'ep'), None)
    col_spec = P('ep', None, 'etp')
    in_specs = (row_spec, row_spec, row_spec, row_spec, col_spec, col_spec, P('ep', 'etp', None))
    n_q = mesh.shape['etp']
    group = mesh.shape['ep']

    def device_step(hidden, expert_ids, gate_wts, slot_pos, w_gate, w_up, w_down):
        rows_dev, d_model = hidden.shape
        top_k = expert_ids.shape[1]
        n_e, _, width = w_gate.shape
        rows = rows_dev // n_q
        nx = group // 2
        f32, bf16, i32 = jnp.float32, jnp.bfloat16, jnp.int32
        wide = [k * (d_model // 8) for k in EIGHTHS]
        chunked = [pltpu.VMEM((n_e, n_q, width, w), bf16) for w in wide]
        chunked += [pltpu.VMEM((nx, rows, w) if n < len(wide) - 1 else (8, 128), f32) for n, w in enumerate(wide)]
        chunked += [pltpu.VMEM((2, rows // 2, w), f32) for w in wide]
        chunked += [pltpu.VMEM((2, rows, w), f32) for w in wide]
        return pl.pallas_call(
            functools.partial(moe_kernel, n_q, group),
            out_shape=pltpu.VMEM((rows_dev, d_model), bf16),
            in_specs=[pl.BlockSpec(memory_space=pl.ANY)] * 7,
            out_specs=pl.BlockSpec(memory_space=pltpu.VMEM),
            scratch_shapes=[
                pltpu.VMEM((group, rows, d_model), bf16),
                pltpu.VMEM((group, top_k, rows), i32),
                pltpu.VMEM((group, top_k, rows), f32),
                pltpu.VMEM((group, top_k, rows), i32),
                pltpu.VMEM((group, rows, top_k), f32),
                pltpu.VMEM((n_e, n_q, d_model, 2 * width), bf16),
                pltpu.VMEM((group * n_e, rows, n_q * width), bf16),
                pltpu.VMEM((nx, rows, max(wide)), f32),
                pltpu.VMEM((2, nx, rows, max(wide)), f32),
                *chunked,
                pltpu.SemaphoreType.DMA((152,)),
                pltpu.SemaphoreType.DMA((152,)),
                pltpu.SemaphoreType.DMA((24,)),
                pltpu.SemaphoreType.REGULAR((2,)),
            ],
            compiler_params=pltpu.CompilerParams(collective_id=0, has_side_effects=True, vmem_limit_bytes=59 * 1024 * 1024),
        )(hidden, expert_ids.T, gate_wts.T, slot_pos.T, w_gate, w_up, w_down)

    return jax.shard_map(device_step, mesh=mesh, in_specs=in_specs, out_specs=row_spec, check_vma=False)
```

```python
import functools

import jax
import jax.numpy as jnp
from jax import lax
from jax.experimental import pallas as pl
from jax.experimental.pallas import tpu as pltpu
from jax.sharding import PartitionSpec as P

MESH = pl.DeviceIdType.MESH
EIGHTHS = (1, 1, 2, 2, 1, 1)


def moe_kernel(n_q, group, hid, ids, gts, pos, wg, wu, wd, out, tok, ids_v, gts_v, pos_v, gcol, wgu, act, spart, pr, *rest):
    n_c = len(EIGHTHS)
    wdn, acc, r1, r2 = (list(rest[i * n_c:(i + 1) * n_c]) for i in range(4))
    ssem, rsem, lsem, credit = rest[4 * n_c:]
    rows, d_model = tok.shape[1:]
    n_e, width = wg.shape[0], wg.shape[2]
    nx = group // 2
    hr, hk, he = rows // 2, d_model // 2, n_e // 2
    wide = [k * (d_model // 8) for k in EIGHTHS]
    acc[n_c - 2], acc[n_c - 1] = acc[0], acc[1]
    cols = [slice(sum(wide[:n]), sum(wide[:n + 1])) for n in range(n_c)]
    q, ep = lax.axis_index('etp'), lax.axis_index('ep')
    x, c = lax.div(ep, 2), lax.rem(ep, 2)
    yl, yr = lax.rem(q + n_q - 1, n_q), lax.rem(q + 1, n_q)
    xl, xr, xf = lax.rem(x + nx - 1, nx), lax.rem(x + 1, nx), lax.rem(x + 2, nx)
    bl, br, bf = xl * 2 + c, xr * 2 + c, xf * 2 + c
    to_l, to_r, to_p = {'ep': bl}, {'ep': br}, {'ep': x * 2 + 1 - c}
    up_l, up_r = {'etp': yl}, {'etp': yr}
    used = [0, 0]
    sends = []

    def remote(src, dst, dev):
        k = used[0]
        used[0] += 1
        cp = pltpu.make_async_remote_copy(src_ref=src, dst_ref=dst, send_sem=ssem.at[k], recv_sem=rsem.at[k], device_id=dev, device_id_type=MESH)
        cp.start()
        sends.append(cp)
        return cp

    def local(src, dst):
        k = used[1]
        used[1] += 1
        cp = pltpu.make_async_copy(src, dst, lsem.at[k])
        cp.start()
        return cp

    def arrive(cps):
        for cp in cps:
            cp.wait_recv()

    barrier = pltpu.get_barrier_semaphore()
    for dev in (to_l, to_r, to_p, up_l, up_r):
        pl.semaphore_signal(barrier, inc=1, device_id=dev, device_id_type=MESH)

    start = pl.multiple_of(q * rows, rows)
    route = [(a.at[:, pl.ds(start, rows)], v) for a, v in ((ids, ids_v), (gts, gts_v), (pos, pos_v))]

    def load_gu(e):
        return [local(wg.at[e], wgu.at[e, 0, :, 0:width]), local(wu.at[e], wgu.at[e, 0, :, width:2 * width])]

    mine_gu = {0: load_gu(0)}
    mine_tok = [local(hid.at[pl.ds(start, rows)], tok.at[ep])] + [local(a, v.at[ep]) for a, v in route]
    for e in range(1, n_e):
        mine_gu[e] = load_gu(e)
    mine_dn = [local(wd.at[:, :, cols[n]], wdn[n].at[:, 0]) for n in range(n_c)]
    pl.semaphore_wait(barrier, 5)

    def send_gu(e):
        if e < 2:
            for cp in mine_gu[e]:
                cp.wait()
        return [remote(wgu.at[e, 0], wgu.at[e, slot], dev) for slot, dev in ((1, up_r), (2, up_l))]

    def pass_gu(e, cps):
        arrive(cps)
        return [
            remote(wgu.at[e, 1, 0:hk], wgu.at[e, 3, 0:hk], up_r),
            remote(wgu.at[e, 2, hk:d_model], wgu.at[e, 3, hk:d_model], up_l),
        ]

    def send_dn(n):
        mine_dn[n].wait()
        return [remote(wdn[n].at[:, 0], wdn[n].at[:, slot], dev) for slot, dev in ((1, up_r), (2, up_l))]

    def pass_dn(n, cps):
        arrive(cps)
        return [
            remote(wdn[n].at[0:he, 1], wdn[n].at[0:he, 3], up_r),
            remote(wdn[n].at[he:n_e, 2], wdn[n].at[he:n_e, 3], up_l),
        ]

    def send_tok(dev):
        return [remote(tok.at[ep], tok.at[ep], dev)] + pass_route(ep, dev)

    def pass_route(b, dev):
        return [remote(v.at[b], v.at[b], dev) for v in (ids_v, gts_v, pos_v)]

    gu = {0: send_gu(0)}
    for cp in mine_tok:
        cp.wait()
    tok_r, tok_l, tok_p = send_tok(to_r), send_tok(to_l), send_tok(to_p)
    gu[1] = send_gu(1)

    def block_at(o):
        h = lax.div(o, 2)
        xi = lax.rem(x + h + lax.div(h, 2) - 2 * lax.div(h, 3), nx)
        return xi * 2 + lax.rem(o, 2)

    def make_gates(lo, hi):
        def body(o, carry):
            b = block_at(o)
            weight = jnp.where(pos_v[b] >= 0, gts_v[b], 0.0)
            chosen = ids_v[b]
            line = lax.broadcasted_iota(jnp.int32, weight.shape, 0)
            table = jnp.zeros_like(weight)
            for e in range(n_e):
                one = jnp.sum(jnp.where(chosen == ep * n_e + e, weight, 0.0), axis=0, keepdims=True)
                table = jnp.where(line == e, one, table)
            gcol[b] = table.T
            return carry

        lax.fori_loop(lo, hi, body, 0)

    def up(e0, e1, slots, lo, hi):
        span = e1 - e0
        total = (hi - lo) * span
        step = max(span, 4 // len(slots))
        while total % step:
            step -= 1

        def body(i, carry):
            for k in range(step):
                b, e = block_at(lo + i * (step // span) + k // span), e0 + k % span
                gate = gcol[b, :, e:e + 1]
                for s in slots:
                    prod = jnp.dot(tok[b], wgu[e, s], preferred_element_type=jnp.float32)
                    h = jnp.where(gate > 0, jax.nn.silu(prod[:, :width]) * prod[:, width:], 0.0)
                    act[b * n_e + e, :, s * width:(s + 1) * width] = h.astype(jnp.bfloat16)
            return carry

        lax.fori_loop(0, total // step, body, 0)

    fwd, dn, fdn = {}, {}, {}
    for e in range(2, n_e):
        for cp in mine_gu[e]:
            cp.wait()
    arrive(tok_p)
    make_gates(0, 2)
    up(0, n_e, (0,), 0, 2)
    fwd[0] = pass_gu(0, gu[0])
    gu[2] = send_gu(2)
    up(0, 1, (1, 2), 0, 2)
    fwd[1] = pass_gu(1, gu[1])
    gu[3] = send_gu(3)
    up(1, 2, (1, 2), 0, 2)
    arrive(tok_r)
    arrive(tok_l)
    relay = [remote(tok.at[b], tok.at[b], to_p) for b in (bl, br)]
    far = [
        remote(tok.at[bl, 0:hr], tok.at[bl, 0:hr], to_r),
        remote(tok.at[br, hr:rows], tok.at[br, hr:rows], to_l),
    ]
    relay += pass_route(bl, to_p) + pass_route(br, to_p)
    far += pass_route(bl, to_r)
    arrive(relay)
    make_gates(2, 6)
    up(0, n_e, (0,), 2, 6)
    up(0, 2, (1, 2), 2, 6)
    arrive(far)
    relay = [remote(tok.at[bf], tok.at[bf], to_p)] + pass_route(bf, to_p)
    arrive(fwd[0])
    up(0, 1, (3,), 0, 6)
    fwd[2] = pass_gu(2, gu[2])
    dn[0] = send_dn(0)
    arrive(relay)
    make_gates(6, 8)
    up(0, n_e, (0,), 6, 8)
    up(0, 2, (1, 2), 6, 8)
    up(0, 1, (3,), 6, 8)
    up(2, 3, (1, 2), 0, 8)
    arrive(fwd[1])
    up(1, 2, (3,), 0, 8)
    fwd[3] = pass_gu(3, gu[3])
    up(3, 4, (1, 2), 0, 8)
    arrive(fwd[2])
    up(2, 3, (3,), 0, 8)
    fdn[0] = pass_dn(0, dn[0])
    dn[1] = send_dn(1)
    arrive(fwd[3])
    up(3, 4, (3,), 0, 8)

    def down(n, b, dst):
        for e in range(n_e):
            mat = wdn[n][e].reshape(n_q * width, wide[n])
            term = gcol[b, :, e:e + 1] * jnp.dot(act[b * n_e + e], mat, preferred_element_type=jnp.float32)
            if e == 0:
                dst[...] = term
            else:
                dst[...] += term

    first, second, outs, fouts = {}, {}, {}, {}

    d2d_base, used[0] = used[0], used[0] + nx * n_c

    def to_partner(n, i):
        xi, k = lax.rem(xf + i, nx), d2d_base + n * nx + i
        return pltpu.make_async_remote_copy(
            src_ref=spart.at[xi, :, 0:wide[n]], dst_ref=pr.at[n % 2, xi, :, 0:wide[n]],
            send_sem=ssem.at[k], recv_sem=rsem.at[k], device_id=to_p, device_id_type=MESH)

    def products(n, lo, hi):
        def body(i, carry):
            xi = lax.rem(xf + i, nx)
            down(n, xi * 2 + 1 - c, spart.at[xi, :, 0:wide[n]])
            to_partner(n, i).start()
            down(n, xi * 2 + c, acc[n].at[xi])
            return carry

        lax.fori_loop(lo, hi, body, 0)

    def join(n, i):
        to_partner(n, i).wait_recv()
        xi = lax.rem(xf + i, nx)
        acc[n][xi] += pr[n % 2, xi, :, 0:wide[n]]

    def phase_ab(n, hook=None):
        arrive(fdn[n])
        if n >= 1:
            for i in range(nx):
                to_partner(n - 1, i).wait_send()
        if n >= n_c - 2:
            drained = first[n - n_c + 2] + second[n - n_c + 2]
            for cp in drained:
                cp.wait_send()
            sends[:] = [cp for cp in sends if not any(cp is old for old in drained)]
        if n >= 2:
            pl.semaphore_wait(credit.at[n % 2], 1)
        early = 1 if n < 3 else nx
        products(n, 0, early)
        join(n, 0)
        first[n] = [
            remote(acc[n].at[xf, 0:hr], r1[n].at[0], to_r),
            remote(acc[n].at[xf, hr:rows], r1[n].at[1], to_l),
        ]
        if hook is not None:
            hook()
        if early < nx:
            products(n, early, nx)
        join(n, 1)
        second[n] = [remote(acc[n].at[xl, 0:hr], r2[n].at[1, 0:hr], to_l)]
        join(n, 3)
        second[n].append(remote(acc[n].at[xr, hr:rows], r2[n].at[0, hr:rows], to_r))
        join(n, 2)
        if n + 2 < n_c:
            pl.semaphore_signal(credit.at[n % 2], inc=1, device_id=to_p, device_id_type=MESH)

    def phase_c(n):
        first[n][0].wait_recv()
        acc[n][xr, 0:hr] += r1[n][0]
        second[n].append(remote(acc[n].at[xr, 0:hr], r2[n].at[0, 0:hr], to_r))
        first[n][1].wait_recv()
        acc[n][xl, hr:rows] += r1[n][1]
        second[n].append(remote(acc[n].at[xl, hr:rows], r2[n].at[1, hr:rows], to_l))

    def place(n, quarter, lo, hi):
        return out.at[pl.ds(pl.multiple_of(quarter * rows + lo, hr), hi - lo), cols[n]]

    def phase_d(n):
        arrive(second[n])
        total = acc[n][x] + r2[n][0] + r2[n][1]
        out[pl.ds(start, rows), cols[n]] = total.astype(jnp.bfloat16)
        low, high = place(n, q, 0, hr), place(n, q, hr, rows)
        outs[n] = [remote(low, low, up_r), remote(high, high, up_l), remote(high, high, up_r), remote(low, low, up_l)]

    def phase_e(n):
        arrive(outs[n][:2])
        fouts[n] = [
            remote(place(n, yl, 0, hr), place(n, yl, 0, hr), up_r),
            remote(place(n, yr, hr, rows), place(n, yr, hr, rows), up_l),
        ]

    def pass_on(n, *later):
        fdn[n] = pass_dn(n, dn[n])
        for k in later:
            dn[k] = send_dn(k)

    phase_ab(0, lambda: pass_on(1, 2))
    phase_ab(1, lambda: phase_c(0))
    pass_on(2, 3)
    phase_c(1)
    phase_ab(2, lambda: phase_d(0))
    pass_on(3, 4, 5)
    phase_d(1)
    phase_c(2)
    phase_ab(3)
    pass_on(4)
    phase_e(0)
    phase_e(1)
    phase_ab(4)
    pass_on(5)
    phase_d(2)
    phase_c(3)
    phase_ab(5)
    phase_e(2)
    phase_c(4)
    phase_d(3)
    phase_e(3)
    phase_c(5)
    phase_d(4)
    phase_e(4)
    phase_d(5)
    phase_e(5)
    for i in range(nx):
        to_partner(n_c - 1, i).wait_send()
    for n in range(n_c):
        arrive(outs[n][2:] + fouts[n])
    for cp in sends:
        cp.wait_send()


def solution(mesh):
    row_spec = P(('dp', 'ep'), None)
    col_spec = P('ep', None, 'etp')
    in_specs = (row_spec, row_spec, row_spec, row_spec, col_spec, col_spec, P('ep', 'etp', None))
    n_q = mesh.shape['etp']
    group = mesh.shape['ep']

    def device_step(hidden, expert_ids, gate_wts, slot_pos, w_gate, w_up, w_down):
        rows_dev, d_model = hidden.shape
        top_k = expert_ids.shape[1]
        n_e, _, width = w_gate.shape
        rows = rows_dev // n_q
        nx = group // 2
        f32, bf16, i32 = jnp.float32, jnp.bfloat16, jnp.int32
        wide = [k * (d_model // 8) for k in EIGHTHS]
        chunked = [pltpu.VMEM((n_e, n_q, width, w), bf16) for w in wide]
        chunked += [pltpu.VMEM((nx, rows, w) if n < len(wide) - 2 else (8, 128), f32) for n, w in enumerate(wide)]
        chunked += [pltpu.VMEM((2, rows // 2, w), f32) for w in wide]
        chunked += [pltpu.VMEM((2, rows, w), f32) for w in wide]
        return pl.pallas_call(
            functools.partial(moe_kernel, n_q, group),
            out_shape=pltpu.VMEM((rows_dev, d_model), bf16),
            in_specs=[pl.BlockSpec(memory_space=pl.ANY)] * 7,
            out_specs=pl.BlockSpec(memory_space=pltpu.VMEM),
            scratch_shapes=[
                pltpu.VMEM((group, rows, d_model), bf16),
                pltpu.VMEM((group, top_k, rows), i32),
                pltpu.VMEM((group, top_k, rows), f32),
                pltpu.VMEM((group, top_k, rows), i32),
                pltpu.VMEM((group, rows, top_k), f32),
                pltpu.VMEM((n_e, n_q, d_model, 2 * width), bf16),
                pltpu.VMEM((group * n_e, rows, n_q * width), bf16),
                pltpu.VMEM((nx, rows, max(wide)), f32),
                pltpu.VMEM((2, nx, rows, max(wide)), f32),
                *chunked,
                pltpu.SemaphoreType.DMA((168,)),
                pltpu.SemaphoreType.DMA((168,)),
                pltpu.SemaphoreType.DMA((24,)),
                pltpu.SemaphoreType.REGULAR((2,)),
            ],
            compiler_params=pltpu.CompilerParams(collective_id=0, has_side_effects=True, vmem_limit_bytes=59 * 1024 * 1024),
        )(hidden, expert_ids.T, gate_wts.T, slot_pos.T, w_gate, w_up, w_down)

    return jax.shard_map(device_step, mesh=mesh, in_specs=in_specs, out_specs=row_spec, check_vma=False)
```

```python
import functools

import jax
import jax.numpy as jnp
from jax import lax
from jax.experimental import pallas as pl
from jax.experimental.pallas import tpu as pltpu
from jax.sharding import PartitionSpec as P

MESH = pl.DeviceIdType.MESH
EIGHTHS = (2, 2, 2, 1, 1)


def moe_kernel(n_q, group, hid, ids, gts, pos, wg, wu, wd, out, tok, ids_v, gts_v, pos_v, gcol, wgu, act, spart, pr, *rest):
    n_c = len(EIGHTHS)
    wdn, acc, r1, r2 = (list(rest[i * n_c:(i + 1) * n_c]) for i in range(4))
    ssem, rsem, lsem, credit = rest[4 * n_c:]
    rows, d_model = tok.shape[1:]
    n_e, width = wg.shape[0], wg.shape[2]
    nx = group // 2
    hr, hk, he = rows // 2, d_model // 2, n_e // 2
    wide = [k * (d_model // 8) for k in EIGHTHS]
    acc[n_c - 1] = acc[0].at[:, :, 0:wide[-1]]
    cols = [slice(sum(wide[:n]), sum(wide[:n + 1])) for n in range(n_c)]
    q, ep = lax.axis_index('etp'), lax.axis_index('ep')
    x, c = lax.div(ep, 2), lax.rem(ep, 2)
    yl, yr = lax.rem(q + n_q - 1, n_q), lax.rem(q + 1, n_q)
    xl, xr, xf = lax.rem(x + nx - 1, nx), lax.rem(x + 1, nx), lax.rem(x + 2, nx)
    bl, br, bf = xl * 2 + c, xr * 2 + c, xf * 2 + c
    to_l, to_r, to_p = {'ep': bl}, {'ep': br}, {'ep': x * 2 + 1 - c}
    up_l, up_r = {'etp': yl}, {'etp': yr}
    used = [0, 0]
    sends = []

    def remote(src, dst, dev):
        k = used[0]
        used[0] += 1
        cp = pltpu.make_async_remote_copy(src_ref=src, dst_ref=dst, send_sem=ssem.at[k], recv_sem=rsem.at[k], device_id=dev, device_id_type=MESH)
        cp.start()
        sends.append(cp)
        return cp

    def local(src, dst):
        k = used[1]
        used[1] += 1
        cp = pltpu.make_async_copy(src, dst, lsem.at[k])
        cp.start()
        return cp

    def arrive(cps):
        for cp in cps:
            cp.wait_recv()

    barrier = pltpu.get_barrier_semaphore()
    for dev in (to_l, to_r, to_p, up_l, up_r):
        pl.semaphore_signal(barrier, inc=1, device_id=dev, device_id_type=MESH)

    start = pl.multiple_of(q * rows, rows)
    route = [(a.at[:, pl.ds(start, rows)], v) for a, v in ((ids, ids_v), (gts, gts_v), (pos, pos_v))]

    def load_gu(e):
        return [local(wg.at[e], wgu.at[e, 0, :, 0:width]), local(wu.at[e], wgu.at[e, 0, :, width:2 * width])]

    mine_gu = {0: load_gu(0)}
    mine_tok = [local(hid.at[pl.ds(start, rows)], tok.at[ep])] + [local(a, v.at[ep]) for a, v in route]
    for e in range(1, n_e):
        mine_gu[e] = load_gu(e)
    mine_dn = [local(wd.at[:, :, cols[n]], wdn[n].at[:, 0]) for n in range(n_c)]
    pl.semaphore_wait(barrier, 5)

    def send_gu(e):
        if e < 2:
            for cp in mine_gu[e]:
                cp.wait()
        return [remote(wgu.at[e, 0], wgu.at[e, slot], dev) for slot, dev in ((1, up_r), (2, up_l))]

    def pass_gu(e, cps):
        arrive(cps)
        return [
            remote(wgu.at[e, 1, 0:hk], wgu.at[e, 3, 0:hk], up_r),
            remote(wgu.at[e, 2, hk:d_model], wgu.at[e, 3, hk:d_model], up_l),
        ]

    def send_dn(n):
        mine_dn[n].wait()
        return [remote(wdn[n].at[:, 0], wdn[n].at[:, slot], dev) for slot, dev in ((1, up_r), (2, up_l))]

    def pass_dn(n, cps):
        arrive(cps)
        return [
            remote(wdn[n].at[0:he, 1], wdn[n].at[0:he, 3], up_r),
            remote(wdn[n].at[he:n_e, 2], wdn[n].at[he:n_e, 3], up_l),
        ]

    def send_tok(dev):
        return [remote(tok.at[ep], tok.at[ep], dev)] + pass_route(ep, dev)

    def pass_route(b, dev):
        return [remote(v.at[b], v.at[b], dev) for v in (ids_v, gts_v, pos_v)]

    gu = {0: send_gu(0)}
    for cp in mine_tok:
        cp.wait()
    tok_r, tok_l, tok_p = send_tok(to_r), send_tok(to_l), send_tok(to_p)
    gu[1] = send_gu(1)

    def block_at(o):
        h = lax.div(o, 2)
        xi = lax.rem(x + h + lax.div(h, 2) - 2 * lax.div(h, 3), nx)
        return xi * 2 + lax.rem(o, 2)

    def make_gates(lo, hi):
        def body(o, carry):
            b = block_at(o)
            weight = jnp.where(pos_v[b] >= 0, gts_v[b], 0.0)
            chosen = ids_v[b]
            line = lax.broadcasted_iota(jnp.int32, weight.shape, 0)
            table = jnp.zeros_like(weight)
            for e in range(n_e):
                one = jnp.sum(jnp.where(chosen == ep * n_e + e, weight, 0.0), axis=0, keepdims=True)
                table = jnp.where(line == e, one, table)
            gcol[b] = table.T
            return carry

        lax.fori_loop(lo, hi, body, 0)

    def up(e0, e1, slots, lo, hi):
        span = e1 - e0
        total = (hi - lo) * span
        step = max(span, 4 // len(slots))
        while total % step:
            step -= 1

        def body(i, carry):
            for k in range(step):
                b, e = block_at(lo + i * (step // span) + k // span), e0 + k % span
                gate = gcol[b, :, e:e + 1]
                for s in slots:
                    prod = jnp.dot(tok[b], wgu[e, s], preferred_element_type=jnp.float32)
                    h = jnp.where(gate > 0, jax.nn.silu(prod[:, :width]) * prod[:, width:], 0.0)
                    act[b * n_e + e, :, s * width:(s + 1) * width] = h.astype(jnp.bfloat16)
            return carry

        lax.fori_loop(0, total // step, body, 0)

    fwd, dn, fdn = {}, {}, {}
    for e in range(2, n_e):
        for cp in mine_gu[e]:
            cp.wait()
    arrive(tok_p)
    make_gates(0, 2)
    up(0, n_e, (0,), 0, 2)
    fwd[0] = pass_gu(0, gu[0])
    gu[2] = send_gu(2)
    up(0, 1, (1, 2), 0, 2)
    fwd[1] = pass_gu(1, gu[1])
    gu[3] = send_gu(3)
    up(1, 2, (1, 2), 0, 2)
    arrive(tok_r)
    arrive(tok_l)
    relay = [remote(tok.at[b], tok.at[b], to_p) for b in (bl, br)]
    far = [
        remote(tok.at[bl, 0:hr], tok.at[bl, 0:hr], to_r),
        remote(tok.at[br, hr:rows], tok.at[br, hr:rows], to_l),
    ]
    relay += pass_route(bl, to_p) + pass_route(br, to_p)
    far += pass_route(bl, to_r)
    arrive(relay)
    make_gates(2, 6)
    up(0, n_e, (0,), 2, 6)
    up(0, 2, (1, 2), 2, 6)
    arrive(far)
    relay = [remote(tok.at[bf], tok.at[bf], to_p)] + pass_route(bf, to_p)
    arrive(fwd[0])
    up(0, 1, (3,), 0, 6)
    fwd[2] = pass_gu(2, gu[2])
    dn[0] = send_dn(0)
    arrive(relay)
    make_gates(6, 8)
    up(0, n_e, (0,), 6, 8)
    up(0, 2, (1, 2), 6, 8)
    up(0, 1, (3,), 6, 8)
    up(2, 3, (1, 2), 0, 8)
    arrive(fwd[1])
    up(1, 2, (3,), 0, 8)
    fwd[3] = pass_gu(3, gu[3])
    up(3, 4, (1, 2), 0, 8)
    arrive(fwd[2])
    up(2, 3, (3,), 0, 8)
    fdn[0] = pass_dn(0, dn[0])
    dn[1] = send_dn(1)
    arrive(fwd[3])
    up(3, 4, (3,), 0, 8)

    def down(n, b, dst):
        for e in range(n_e):
            mat = wdn[n][e].reshape(n_q * width, wide[n])
            term = gcol[b, :, e:e + 1] * jnp.dot(act[b * n_e + e], mat, preferred_element_type=jnp.float32)
            if e == 0:
                dst[...] = term
            else:
                dst[...] += term

    first, second, late, outs, fouts = {}, {}, {}, {}, {}
    parts = [1] * (n_c - 1) + [2]

    d2d_base, used[0] = used[0], used[0] + nx * n_c

    def to_partner(n, i):
        xi, k = lax.rem(xf + i, nx), d2d_base + n * nx + i
        return pltpu.make_async_remote_copy(
            src_ref=spart.at[xi, :, 0:wide[n]], dst_ref=pr.at[n % 2, xi, :, 0:wide[n]],
            send_sem=ssem.at[k], recv_sem=rsem.at[k], device_id=to_p, device_id_type=MESH)

    def products(n, lo, hi):
        def body(i, carry):
            xi = lax.rem(xf + i, nx)
            down(n, xi * 2 + 1 - c, spart.at[xi, :, 0:wide[n]])
            to_partner(n, i).start()
            down(n, xi * 2 + c, acc[n].at[xi])
            return carry

        lax.fori_loop(lo, hi, body, 0)

    def join(n, i):
        to_partner(n, i).wait_recv()
        xi = lax.rem(xf + i, nx)
        acc[n][xi] += pr[n % 2, xi, :, 0:wide[n]]

    def phase_ab(n):
        arrive(fdn[n])
        if n >= 1:
            for i in range(nx):
                to_partner(n - 1, i).wait_send()
        if n == n_c - 1:
            drained = first[0] + second[0] + sum(late[0], [])
            for cp in drained:
                cp.wait_send()
            sends[:] = [cp for cp in sends if not any(cp is old for old in drained)]
        if n >= 2:
            pl.semaphore_wait(credit.at[n % 2], 1)
        early = 2 if n == 0 else nx
        products(n, 0, early)
        join(n, 0)
        first[n] = [
            remote(acc[n].at[xf, 0:hr], r1[n].at[0], to_r),
            remote(acc[n].at[xf, hr:rows], r1[n].at[1], to_l),
        ]
        if early < nx:
            products(n, early, nx)
        join(n, 1)
        second[n] = [remote(acc[n].at[xl, 0:hr], r2[n].at[1, 0:hr], to_l)]
        join(n, 3)
        second[n].append(remote(acc[n].at[xr, hr:rows], r2[n].at[0, hr:rows], to_r))
        join(n, 2)
        if n + 2 < n_c:
            pl.semaphore_signal(credit.at[n % 2], inc=1, device_id=to_p, device_id_type=MESH)

    def phase_c(n):
        first[n][0].wait_recv()
        acc[n][xr, 0:hr] += r1[n][0]
        size = hr // parts[n]
        late[n] = [[remote(acc[n].at[xr, p * size:(p + 1) * size], r2[n].at[0, p * size:(p + 1) * size], to_r)] for p in range(parts[n])]
        first[n][1].wait_recv()
        acc[n][xl, hr:rows] += r1[n][1]
        for p in range(parts[n]):
            lo, hi = hr + p * size, hr + (p + 1) * size
            late[n][p].append(remote(acc[n].at[xl, lo:hi], r2[n].at[1, lo:hi], to_l))

    def place(n, quarter, lo, hi):
        return out.at[pl.ds(pl.multiple_of(quarter * rows + lo, hr // 2), hi - lo), cols[n]]

    def bands(n, p):
        size = hr // parts[n]
        return [(lo, lo + size) for lo in (p * size, hr + p * size)]

    def phase_d(n, p=0):
        if p == 0:
            arrive(second[n])
        arrive(late[n][p])
        for lo, hi in bands(n, p):
            total = acc[n][x, lo:hi] + r2[n][0, lo:hi] + r2[n][1, lo:hi]
            out[pl.ds(pl.multiple_of(start + lo, hr // 2), hi - lo), cols[n]] = total.astype(jnp.bfloat16)
        low, high = (place(n, q, lo, hi) for lo, hi in bands(n, p))
        outs[n, p] = [remote(low, low, up_r), remote(high, high, up_l), remote(high, high, up_r), remote(low, low, up_l)]

    def phase_e(n, p=0):
        arrive(outs[n, p][:2])
        (a, b), (c0, c1) = bands(n, p)
        fouts[n, p] = [
            remote(place(n, yl, a, b), place(n, yl, a, b), up_r),
            remote(place(n, yr, c0, c1), place(n, yr, c0, c1), up_l),
        ]

    phase_ab(0)
    fdn[1] = pass_dn(1, dn[1])
    dn[2] = send_dn(2)
    phase_c(0)
    phase_ab(1)
    fdn[2] = pass_dn(2, dn[2])
    dn[3] = send_dn(3)
    dn[4] = send_dn(4)
    phase_ab(2)
    fdn[3] = pass_dn(3, dn[3])
    phase_c(1)
    phase_d(0)
    phase_ab(3)
    fdn[4] = pass_dn(4, dn[4])
    phase_c(2)
    phase_d(1)
    phase_e(0)
    phase_ab(4)
    phase_c(3)
    phase_d(2)
    phase_e(1)
    phase_c(4)
    phase_d(3)
    phase_e(2)
    phase_d(4)
    phase_e(3)
    phase_d(4, 1)
    phase_e(4)
    phase_e(4, 1)
    for i in range(nx):
        to_partner(n_c - 1, i).wait_send()
    for key in sorted(outs):
        arrive(outs[key][2:] + fouts[key])
    for cp in sends:
        cp.wait_send()


def solution(mesh):
    row_spec = P(('dp', 'ep'), None)
    col_spec = P('ep', None, 'etp')
    in_specs = (row_spec, row_spec, row_spec, row_spec, col_spec, col_spec, P('ep', 'etp', None))
    n_q = mesh.shape['etp']
    group = mesh.shape['ep']

    def device_step(hidden, expert_ids, gate_wts, slot_pos, w_gate, w_up, w_down):
        rows_dev, d_model = hidden.shape
        top_k = expert_ids.shape[1]
        n_e, _, width = w_gate.shape
        rows = rows_dev // n_q
        nx = group // 2
        f32, bf16, i32 = jnp.float32, jnp.bfloat16, jnp.int32
        wide = [k * (d_model // 8) for k in EIGHTHS]
        chunked = [pltpu.VMEM((n_e, n_q, width, w), bf16) for w in wide]
        chunked += [pltpu.VMEM((nx, rows, w) if n < len(wide) - 1 else (8, 128), f32) for n, w in enumerate(wide)]
        chunked += [pltpu.VMEM((2, rows // 2, w), f32) for w in wide]
        chunked += [pltpu.VMEM((2, rows, w), f32) for w in wide]
        return pl.pallas_call(
            functools.partial(moe_kernel, n_q, group),
            out_shape=pltpu.VMEM((rows_dev, d_model), bf16),
            in_specs=[pl.BlockSpec(memory_space=pl.ANY)] * 7,
            out_specs=pl.BlockSpec(memory_space=pltpu.VMEM),
            scratch_shapes=[
                pltpu.VMEM((group, rows, d_model), bf16),
                pltpu.VMEM((group, top_k, rows), i32),
                pltpu.VMEM((group, top_k, rows), f32),
                pltpu.VMEM((group, top_k, rows), i32),
                pltpu.VMEM((group, rows, top_k), f32),
                pltpu.VMEM((n_e, n_q, d_model, 2 * width), bf16),
                pltpu.VMEM((group * n_e, rows, n_q * width), bf16),
                pltpu.VMEM((nx, rows, max(wide)), f32),
                pltpu.VMEM((2, nx, rows, max(wide)), f32),
                *chunked,
                pltpu.SemaphoreType.DMA((164,)),
                pltpu.SemaphoreType.DMA((164,)),
                pltpu.SemaphoreType.DMA((24,)),
                pltpu.SemaphoreType.REGULAR((2,)),
            ],
            compiler_params=pltpu.CompilerParams(collective_id=0, has_side_effects=True, vmem_limit_bytes=59 * 1024 * 1024),
        )(hidden, expert_ids.T, gate_wts.T, slot_pos.T, w_gate, w_up, w_down)

    return jax.shard_map(device_step, mesh=mesh, in_specs=in_specs, out_specs=row_spec, check_vma=False)
```
